128 devices in a mesh: dom: 4 (over y_hi, core), dim: 32 (over z, y_lo, x).
Axes of the slice: x: 4, y: 4 (y_hi: 2, y_lo: 2; y = y_hi * 2 + y_lo), z: 4, core: 2. Of those that a mesh axis runs over, the one named last changes fastest.
Arguments:
- particles: float32 [512, 262144], P('dom', 'dim'), may hold values from -16 to 16
- scores: float32 [512, 262144], P('dom', 'dim'), may hold values from -0.00036621094 to 0.00036621094
- spread: float32 [], replicated, may hold values from 131072 to 262144
- step_size: float32 [], replicated, may hold values from 4194304 to 8388608
Outputs:
- new_particles: float32 [512, 262144], P('dom', 'dim')
The draws below stay inside these ranges and needn't reach their ends.
All inputs are finite; a program needn't handle non-finite values.
Results may differ from the reference program's by a relative error of at most 0.000064.
Values sent between devices are 32-bit elements; how exact they have to be, the bound alone decides.
A program may use at most 128 MiB of HBM per device.

```python
import math
import jax
import jax.numpy as jnp
from jax import lax

D = 262144
P_SIZE = 512


latent_count = 32


def draw_particles(key, part):
    keys = jax.random.split(jax.random.fold_in(key, 11), 7)
    row_low = 0.7
    row_high = 1.4
    smooth_reach = 0.55
    row_scale = jnp.exp(jax.random.uniform(keys[0], (P_SIZE, 1), jnp.float32, math.log(row_low), math.log(row_high)))
    phase = jax.random.uniform(keys[1], (), jnp.float32, 0.0, 2.0 * math.pi)
    position = jnp.arange(D, dtype=jnp.float32) / D
    rough = jnp.exp(jax.random.uniform(keys[2], (1, D), jnp.float32, math.log(0.7), math.log(1.4)))
    column_scale = jnp.exp(smooth_reach * jnp.cos(2.0 * math.pi * position + phase))[None, :] * rough
    center = 1.5 * jnp.clip(jax.random.normal(keys[3], (1, D), jnp.float32), -4.0, 4.0)
    mixing = jax.random.normal(keys[4], (P_SIZE, latent_count), jnp.float32)
    factors = jnp.clip(jax.random.normal(keys[5], (latent_count, D), jnp.float32), -6.0, 6.0)
    noise = jnp.clip(jax.random.normal(keys[6], (P_SIZE, D), jnp.float32), -6.0, 6.0)
    shared = jnp.dot(mixing, factors, precision=lax.Precision.HIGHEST, preferred_element_type=jnp.float32) / math.sqrt(latent_count)
    deviation = math.sqrt(0.75) * shared + 0.5 * noise
    result = center + 0.5 * row_scale * column_scale * deviation
    return jnp.clip(result, -16.0, 16.0).astype(jnp.float32)


def shard_levels(stream_key, extent, cuts, smallest, high):
    factor_of, own = 1.0, jax.random.fold_in(stream_key, 6)
    for dim, parts in cuts:
        heights = jnp.exp(jax.random.uniform(jax.random.fold_in(own, dim), (parts,), jnp.float32, smallest / len(cuts), high / len(cuts)))
        factor_of = factor_of * jnp.repeat(heights, extent[dim] // parts).reshape([-1 if axis == dim else 1 for axis in range(len(extent))])
    return factor_of


def gaussian(key, shape, scale, reach, pieces=(), kind=jnp.bfloat16):
    array = scale * jax.random.normal(key, shape, jnp.float32)
    if pieces:
        array = array * shard_levels(key, shape, pieces, -0.22, 0.18)
    return jnp.clip(array, -reach, reach).astype(kind)


def setup_inputs(seed: int = 0) -> dict:
    streams_of = jax.random.split(jax.random.key(seed), 5)
    particles = draw_particles(jax.random.fold_in(streams_of[4], 71), 0)
    scores = gaussian(streams_of[1], (P_SIZE, D), (16.0 / D), 0.00036621094, ((0, 4), (1, 32)), jnp.float32)
    spread = jnp.clip(jnp.exp(jax.random.uniform(streams_of[2], (), jnp.float32, math.log(131072.0), math.log(262144.0))), 131072.0, 262144.0)
    step_size = jnp.clip(jnp.exp(jax.random.uniform(streams_of[3], (), jnp.float32, math.log(4194304), math.log(8388608))), 4194304, 8388608)
    return dict(particles=particles, scores=scores, spread=spread, step_size=step_size)


def reference(particles, scores, spread, step_size):
    precise = lax.Precision.HIGHEST
    squares = jnp.sum(particles * particles, axis=1)
    gram = jnp.dot(particles, particles.T, precision=precise, preferred_element_type=jnp.float32)
    kernel = jnp.exp(-(squares[:, None] + squares[None, :] - 2.0 * gram) / spread)
    attract = jnp.dot(kernel, scores, precision=precise, preferred_element_type=jnp.float32)
    pulled = jnp.dot(kernel, particles, precision=precise, preferred_element_type=jnp.float32)
    weight_sum = jnp.sum(kernel, axis=1, keepdims=True)
    update = (attract + (2.0 / spread) * (weight_sum * particles - pulled)) / particles.shape[0]
    return particles + step_size * update
```

```python
import functools

import jax
import jax.numpy as jnp
from jax import lax
from jax.experimental import pallas as pl
from jax.experimental.pallas import tpu as pltpu
from jax.sharding import PartitionSpec as P

MESH = pl.DeviceIdType.MESH
PARTS = 4
EARLY = 3


def body(
    size_dom, rows, quarter,
    scal, p_ref, s_ref, out_ref,
    pb, sb, pt, qs, ob, gram, half_in, xin, zin, yin, full, k_own, k_oth, w_ref,
    load_sem, sib_send, sib_recv, p_send, p_recv, s_send, s_recv, q_send, q_recv,
    red_send, red_recv, x_send, x_recv, z_send, z_recv, y_send, y_recv,
    gz_send, gz_recv, gx_send, gx_recv, gc_send, gc_recv,
    o_local, o_send, o_recv,
):
    piece = quarter // PARTS
    dom, dim = lax.axis_index("dom"), lax.axis_index("dim")
    h, c = dom // 2, lax.rem(dom, 2)
    z, lo, x = dim // 8, lax.rem(dim // 4, 2), lax.rem(dim, 4)
    y = h * 2 + lo
    block = dom

    def dev(hh, cc, zz, ll, xx):
        return (hh * 2 + cc, zz * 8 + ll * 4 + xx)

    sib = dev(h, 1 - c, z, lo, x)
    over = [dev(1 - h, cc, z, lo, x) for cc in range(2)]
    xs = [dev(h, c, z, lo, lax.rem(x + d, 4)) for d in (1, 2, 3)]
    zs = [dev(h, c, lax.rem(z + d, 4), lo, x) for d in (1, 2, 3)]
    ys = []
    for d in (1, 2, 3):
        yy = lax.rem(y + d, 4)
        ys.append(dev(yy // 2, c, z, lax.rem(yy, 2), x))
    cross = dev(1 - h, 1 - c, z, lo, x)

    barrier = pltpu.get_barrier_semaphore()
    peers = [sib, cross, *xs, *zs, *ys]
    for peer in peers:
        pl.semaphore_signal(barrier, inc=1, device_id=peer, device_id_type=MESH)
    pl.semaphore_wait(barrier, len(peers))

    def remote(src, dst, ssem, rsem, to):
        return pltpu.make_async_remote_copy(
            src_ref=src, dst_ref=dst, send_sem=ssem, recv_sem=rsem,
            device_id=to, device_id_type=MESH,
        )

    def cols(cc, g, k, width):
        return pl.ds(pl.multiple_of(cc * (2 * quarter) + g * quarter + k * piece, piece), width)

    def mine(b):
        return pl.ds(pl.multiple_of(b * rows, rows), rows)

    def kcols(k):
        return pl.ds(pl.multiple_of(k * piece, piece), piece)

    side = [h, 1 - h]

    def p_copy(cc, k):
        return remote(p_ref.at[:, cols(cc, 1 - h, k, piece)], pb.at[0, mine(block), kcols(k)],
                      p_send.at[cc, k], p_recv.at[c, k], over[cc])

    def s_copy(cc, k):
        return remote(s_ref.at[:, cols(cc, 1 - h, k, piece)], sb.at[0, mine(block), kcols(k)],
                      s_send.at[cc, k], s_recv.at[c, k], over[cc])

    def q_copy(cc, k):
        return remote(qs.at[cc, :, kcols(k)], sb.at[1, mine(block), kcols(k)],
                      q_send.at[cc, k], q_recv.at[c, k], over[cc])

    def arrival(buf, gi, cc, k, ssem, rsem):
        there = buf.at[gi, mine((1 - h) * 2 + cc), kcols(k)]
        return remote(there, there, ssem.at[cc, k], rsem.at[cc, k], over[cc])

    def sib_copy(n, gi):
        src, dst = ((p_ref, pb), (s_ref, sb))[n]
        return remote(src.at[:, cols(1 - c, side[gi], 0, quarter)], dst.at[gi, mine(block), :],
                      sib_send.at[n, gi], sib_recv.at[n, gi], sib)

    for k in range(PARTS):
        for cc in range(2):
            p_copy(cc, k).start()
    loads = []
    for n, (src, dst) in enumerate(((p_ref, pb), (s_ref, sb))):
        for gi in range(2):
            loads.append(pltpu.make_async_copy(
                src.at[:, cols(c, side[gi], 0, quarter)], dst.at[gi, mine(block), :], load_sem.at[2 * n + gi]))
    for cc in range(2):
        loads.append(pltpu.make_async_copy(p_ref.at[:, cols(cc, h, 0, quarter)], pt.at[cc], load_sem.at[4 + cc]))
        loads.append(pltpu.make_async_copy(s_ref.at[:, cols(cc, h, 0, quarter)], qs.at[cc], load_sem.at[6 + cc]))
    for n in range(2):
        for gi in range(2):
            sib_copy(n, gi).start()
    for load in loads:
        load.start()
    for k in range(EARLY):
        for cc in range(2):
            s_copy(cc, k).start()
    for load in loads:
        load.wait()

    spread = jnp.full((1, 128), scal[0], jnp.float32)
    pull = (2.0 / spread)[:, :1]
    for cc in range(2):
        def scale(k, carry, cc=cc):
            qs[cc, :, kcols(k)] = qs[cc, :, kcols(k)] - pull * pt[cc, :, kcols(k)]
            return carry
        lax.fori_loop(0, PARTS, scale, 0)

    sib_copy(0, 0).wait_recv()
    gram[...] = jnp.zeros_like(gram)

    def gram_step(k, carry):
        for cc in range(2):
            arrival(pb, 0, cc, k, p_send, p_recv).wait_recv()
        part = pb[0, :, kcols(k)]
        gram[...] += lax.dot_general(part, part, (((1,), (1,)), ((), ())),
                                     precision=lax.Precision.HIGHEST, preferred_element_type=jnp.float32)
        return carry

    lax.fori_loop(0, PARTS, gram_step, 0)

    count = size_dom * rows
    n_c, n_x, n_z = count // 2, count // 8, count // 32

    def span(start, size):
        return pl.ds(pl.multiple_of(start, size), size)

    copy = remote(gram.at[span((1 - c) * n_c, n_c), :], half_in, red_send, red_recv, sib)
    copy.start()
    copy.wait_recv()
    half_in[...] += gram[span(c * n_c, n_c), :]
    x_copies = [remote(half_in.at[span(lax.rem(x + d, 4) * n_x, n_x), :], xin.at[d - 1],
                       x_send.at[d - 1], x_recv.at[d - 1], xs[d - 1]) for d in (1, 2, 3)]
    for cp in x_copies:
        cp.start()
    for cp in x_copies:
        cp.wait_recv()
    xin[3] = half_in[span(x * n_x, n_x), :] + xin[0] + xin[1] + xin[2]
    z_copies = [remote(xin.at[3, span(lax.rem(z + d, 4) * n_z, n_z), :], zin.at[d - 1],
                       z_send.at[d - 1], z_recv.at[d - 1], zs[d - 1]) for d in (1, 2, 3)]
    for cp in z_copies:
        cp.start()
    for cp in z_copies:
        cp.wait_recv()
    zin[3] = xin[3, span(z * n_z, n_z), :] + zin[0] + zin[1] + zin[2]
    y_copies = [remote(zin.at[3], yin.at[d - 1], y_send.at[d - 1], y_recv.at[d - 1], ys[d - 1]) for d in (1, 2, 3)]
    for cp in y_copies:
        cp.start()
    for k in range(EARLY, PARTS):
        for cc in range(2):
            s_copy(cc, k).start()
    for k in range(PARTS):
        for cc in range(2):
            q_copy(cc, k).start()
    for cp in y_copies:
        cp.wait_recv()
    at_z = span(c * n_c + x * n_x + z * n_z, n_z)
    at_x = span(c * n_c + x * n_x, n_x)
    at_c = span(c * n_c, n_c)
    full[at_z, :] = zin[3] + yin[0] + yin[1] + yin[2]

    gz_copies = [remote(full.at[at_z, :], full.at[at_z, :], gz_send.at[d - 1], gz_recv.at[d - 1], zs[d - 1])
                 for d in (1, 2, 3)]
    for cp in gz_copies:
        cp.start()
    for cp in gz_copies:
        cp.wait_recv()
    gx_copies = [remote(full.at[at_x, :], full.at[at_x, :], gx_send.at[d - 1], gx_recv.at[d - 1], xs[d - 1])
                 for d in (1, 2, 3)]
    for cp in gx_copies:
        cp.start()
    for cp in gx_copies:
        cp.wait_recv()
    gc_copy = remote(full.at[at_c, :], full.at[at_c, :], gc_send, gc_recv, sib)
    gc_copy.start()
    gc_copy.wait_recv()

    pair = 2 * rows
    one = spread[:, :1]

    def diagonal(size, row0, col0, axis):
        tile = full[span(row0, size), :] if axis == 1 else full[...]
        r = lax.broadcasted_iota(jnp.int32, tile.shape, 0) + row0
        q = lax.broadcasted_iota(jnp.int32, tile.shape, 1)
        return jnp.sum(jnp.where(r == q, tile, 0.0), axis=axis, keepdims=True)

    own_sq = diagonal(pair, h * pair, 0, 1)
    all_sq = diagonal(count, 0, 0, 0)
    kern = jnp.exp(-(own_sq + all_sq - 2.0 * full[span(h * pair, pair), :]) / one)
    w_ref[...] = jnp.broadcast_to(jnp.sum(kern, axis=1, keepdims=True), w_ref.shape)
    low, high = kern[:, :pair], kern[:, pair:]
    first = h == 0
    k_own[...] = jnp.where(first, low, high)
    k_oth[...] = jnp.where(first, high, low)

    step = jnp.full((1, 128), scal[1], jnp.float32)[:, :1]
    gain = step / jnp.float32(count)
    keep = 1.0 + gain * pull * w_ref[:, :1]
    own_rows, oth_rows = span(h * pair, pair), span((1 - h) * pair, pair)

    def out_copies(gi, k):
        where = cols(c, side[gi], k, piece)
        local = pltpu.make_async_copy(ob.at[gi, k, mine(c), :], out_ref.at[:, where], o_local.at[gi, k])
        away = remote(ob.at[gi, k, mine(1 - c), :], out_ref.at[:, where], o_send.at[gi, k], o_recv.at[gi, k], sib)
        return local, away

    for gi in range(2):
        sib_copy(1, gi).wait_recv()
        if gi == 1:
            sib_copy(0, 1).wait_recv()

        def update(k, carry, gi=gi):
            for cc in range(2):
                if gi == 0:
                    arrival(sb, 0, cc, k, s_send, s_recv).wait_recv()
                else:
                    arrival(sb, 1, cc, k, q_send, q_recv).wait_recv()
            particles = pb[gi, own_rows, kcols(k)]
            q_own = sb[gi, own_rows, kcols(k)] - pull * particles
            q_oth = sb[gi, oth_rows, kcols(k)]
            if gi == 0:
                q_oth = q_oth - pull * pb[0, oth_rows, kcols(k)]
            total = jnp.dot(k_own[...], q_own, precision=lax.Precision.HIGHEST, preferred_element_type=jnp.float32)
            total += jnp.dot(k_oth[...], q_oth, precision=lax.Precision.HIGHEST, preferred_element_type=jnp.float32)
            ob[gi, k] = keep * particles + gain * total
            local, away = out_copies(gi, k)
            away.start()
            local.start()
            return carry

        lax.fori_loop(0, PARTS, update, 0)

    for k in range(PARTS):
        for cc in range(2):
            p_copy(cc, k).wait_send()
            s_copy(cc, k).wait_send()
            q_copy(cc, k).wait_send()
    for n in range(2):
        for gi in range(2):
            sib_copy(n, gi).wait_send()
    copy.wait_send()
    for cp in (*x_copies, *z_copies, *y_copies, *gz_copies, *gx_copies, gc_copy):
        cp.wait_send()
    for gi in range(2):
        for k in range(PARTS):
            local, away = out_copies(gi, k)
            local.wait()
            away.wait()


def solution(mesh):
    size_dom = mesh.shape["dom"]

    def on_device(particles, scores, spread, step_size):
        rows, width = particles.shape
        quarter = width // 4
        piece = quarter // PARTS
        count = size_dom * rows
        scal = jnp.stack([spread, step_size])
        dma = pltpu.SemaphoreType.DMA
        f32 = jnp.float32
        return pl.pallas_call(
            functools.partial(body, size_dom, rows, quarter),
            out_shape=jax.ShapeDtypeStruct(particles.shape, f32),
            in_specs=[pl.BlockSpec(memory_space=pltpu.SMEM), pl.BlockSpec(memory_space=pl.ANY),
                      pl.BlockSpec(memory_space=pl.ANY)],
            out_specs=pl.BlockSpec(memory_space=pl.ANY),
            scratch_shapes=[
                pltpu.VMEM((2, count, quarter), f32),
                pltpu.VMEM((2, count, quarter), f32),
                pltpu.VMEM((2, rows, quarter), f32),
                pltpu.VMEM((2, rows, quarter), f32),
                pltpu.VMEM((2, PARTS, 2 * rows, piece), f32),
                pltpu.VMEM((count, count), f32),
                pltpu.VMEM((count // 2, count), f32),
                pltpu.VMEM((4, count // 8, count), f32),
                pltpu.VMEM((4, count // 32, count), f32),
                pltpu.VMEM((3, count // 32, count), f32),
                pltpu.VMEM((count, count), f32),
                pltpu.VMEM((2 * rows, 2 * rows), f32),
                pltpu.VMEM((2 * rows, 2 * rows), f32),
                pltpu.VMEM((2 * rows, 128), f32),
                dma((8,)), dma((2, 2)), dma((2, 2)),
                dma((2, PARTS)), dma((2, PARTS)), dma((2, PARTS)), dma((2, PARTS)), dma((2, PARTS)), dma((2, PARTS)),
                dma, dma, dma((3,)), dma((3,)), dma((3,)), dma((3,)), dma((3,)), dma((3,)),
                dma((3,)), dma((3,)), dma((3,)), dma((3,)), dma, dma,
                dma((2, PARTS)), dma((2, PARTS)), dma((2, PARTS)),
            ],
            compiler_params=pltpu.CompilerParams(
                collective_id=0, has_side_effects=True, vmem_limit_bytes=58 << 20),
            name="svgd",
        )(scal, particles, scores)

    return jax.shard_map(
        on_device,
        mesh=mesh,
        in_specs=(P("dom", "dim"), P("dom", "dim"), P(), P()),
        out_specs=P("dom", "dim"),
        check_vma=False,
    )
```

```python
import functools

import jax
import jax.numpy as jnp
from jax import lax
from jax.experimental import pallas as pl
from jax.experimental.pallas import tpu as pltpu
from jax.sharding import PartitionSpec as P

MESH = pl.DeviceIdType.MESH
PARTS = 4
EARLY = 3
LAST = (4, 4, 4, 2, 1, 1)


def body(
    size_dom, rows, quarter,
    spread_ref, step_ref, p_ref, s_ref, out_ref,
    pb, sb, pt, qs, ob, gram, half_in, xin, zin, yin, full, k_own, k_oth, w_ref,
    load_sem, sib_send, sib_recv, p_send, p_recv, s_send, s_recv, q_send, q_recv,
    red_send, red_recv, x_send, x_recv, z_send, z_recv, y_send, y_recv,
    gz_send, gz_recv, gx_send, gx_recv, gc_send, gc_recv,
    o_send, o_recv,
):
    piece, unit = quarter // PARTS, quarter // 16
    dom, dim = lax.axis_index("dom"), lax.axis_index("dim")
    h, c = dom // 2, lax.rem(dom, 2)
    z, lo, x = dim // 8, lax.rem(dim // 4, 2), lax.rem(dim, 4)
    y = h * 2 + lo
    block = dom

    def dev(hh, cc, zz, ll, xx):
        return (hh * 2 + cc, zz * 8 + ll * 4 + xx)

    sib = dev(h, 1 - c, z, lo, x)
    over = [dev(1 - h, cc, z, lo, x) for cc in range(2)]
    xs = [dev(h, c, z, lo, lax.rem(x + d, 4)) for d in (1, 2, 3)]
    zs = [dev(h, c, lax.rem(z + d, 4), lo, x) for d in (1, 2, 3)]
    ys = []
    for d in (1, 2, 3):
        yy = lax.rem(y + d, 4)
        ys.append(dev(yy // 2, c, z, lax.rem(yy, 2), x))
    cross = dev(1 - h, 1 - c, z, lo, x)

    barrier = pltpu.get_barrier_semaphore()
    peers = [sib, cross, *xs, *zs, *ys]
    for peer in peers:
        pl.semaphore_signal(barrier, inc=1, device_id=peer, device_id_type=MESH)
    pl.semaphore_wait(barrier, len(peers))

    def remote(src, dst, ssem, rsem, to):
        return pltpu.make_async_remote_copy(
            src_ref=src, dst_ref=dst, send_sem=ssem, recv_sem=rsem,
            device_id=to, device_id_type=MESH,
        )

    def cols(cc, g, k, width):
        return pl.ds(pl.multiple_of(cc * (2 * quarter) + g * quarter + k * piece, piece), width)

    def mine(b):
        return pl.ds(pl.multiple_of(b * rows, rows), rows)

    def kcols(k):
        return pl.ds(pl.multiple_of(k * piece, piece), piece)

    side = [h, 1 - h]

    def p_copy(cc, k):
        return remote(p_ref.at[:, cols(cc, 1 - h, k, piece)], pb.at[0, mine(block), kcols(k)],
                      p_send.at[cc, k], p_recv.at[c, k], over[cc])

    def s_copy(cc, k):
        return remote(s_ref.at[:, cols(cc, 1 - h, k, piece)], sb.at[0, mine(block), kcols(k)],
                      s_send.at[cc, k], s_recv.at[c, k], over[cc])

    last_at = [pl.ds(unit * sum(LAST[:n]), unit * width) for n, width in enumerate(LAST)]

    def q_copy(cc, n):
        return remote(qs.at[cc, :, last_at[n]], sb.at[1, mine(block), last_at[n]],
                      q_send.at[cc, n], q_recv.at[c, n], over[cc])

    def arrival(buf, gi, cc, k, at, ssem, rsem):
        there = buf.at[gi, mine((1 - h) * 2 + cc), at]
        return remote(there, there, ssem.at[cc, k], rsem.at[cc, k], over[cc])

    def sib_copy(n, gi):
        src, dst = ((p_ref, pb), (s_ref, sb))[n]
        return remote(src.at[:, cols(1 - c, side[gi], 0, quarter)], dst.at[gi, mine(block), :],
                      sib_send.at[n, gi], sib_recv.at[n, gi], sib)

    for k in range(PARTS):
        for cc in range(2):
            p_copy(cc, k).start()
    loads = []
    for n, (src, dst) in enumerate(((p_ref, pb), (s_ref, sb))):
        for gi in range(2):
            loads.append(pltpu.make_async_copy(
                src.at[:, cols(c, side[gi], 0, quarter)], dst.at[gi, mine(block), :], load_sem.at[2 * n + gi]))
    for cc in range(2):
        loads.append(pltpu.make_async_copy(p_ref.at[:, cols(cc, h, 0, quarter)], pt.at[cc], load_sem.at[4 + cc]))
        loads.append(pltpu.make_async_copy(s_ref.at[:, cols(cc, h, 0, quarter)], qs.at[cc], load_sem.at[6 + cc]))
    for n in range(2):
        for gi in range(2):
            sib_copy(n, gi).start()
    for load in loads:
        load.start()
    for k in range(EARLY):
        for cc in range(2):
            s_copy(cc, k).start()
    for load in loads:
        load.wait()

    spread = jnp.full((1, 128), spread_ref[0], jnp.float32)
    pull = (2.0 / spread)[:, :1]
    for cc in range(2):
        def scale(k, carry, cc=cc):
            qs[cc, :, kcols(k)] = qs[cc, :, kcols(k)] - pull * pt[cc, :, kcols(k)]
            return carry
        lax.fori_loop(0, PARTS, scale, 0)

    sib_copy(0, 0).wait_recv()
    gram[...] = jnp.zeros_like(gram)

    def gram_step(k, carry):
        for cc in range(2):
            arrival(pb, 0, cc, k, kcols(k), p_send, p_recv).wait_recv()
        part = pb[0, :, kcols(k)]
        gram[...] += lax.dot_general(part, part, (((1,), (1,)), ((), ())),
                                     precision=lax.Precision.HIGHEST, preferred_element_type=jnp.float32)
        return carry

    lax.fori_loop(0, PARTS, gram_step, 0)

    count = size_dom * rows
    n_c, n_x, n_z = count // 2, count // 8, count // 32

    def span(start, size):
        return pl.ds(pl.multiple_of(start, size), size)

    copy = remote(gram.at[span((1 - c) * n_c, n_c), :], half_in, red_send, red_recv, sib)
    copy.start()
    copy.wait_recv()
    half_in[...] += gram[span(c * n_c, n_c), :]
    x_copies = [remote(half_in.at[span(lax.rem(x + d, 4) * n_x, n_x), :], xin.at[d - 1],
                       x_send.at[d - 1], x_recv.at[d - 1], xs[d - 1]) for d in (1, 2, 3)]
    for cp in x_copies:
        cp.start()
    for cp in x_copies:
        cp.wait_recv()
    xin[3] = half_in[span(x * n_x, n_x), :] + xin[0] + xin[1] + xin[2]
    z_copies = [remote(xin.at[3, span(lax.rem(z + d, 4) * n_z, n_z), :], zin.at[d - 1],
                       z_send.at[d - 1], z_recv.at[d - 1], zs[d - 1]) for d in (1, 2, 3)]
    for cp in z_copies:
        cp.start()
    for cp in z_copies:
        cp.wait_recv()
    zin[3] = xin[3, span(z * n_z, n_z), :] + zin[0] + zin[1] + zin[2]
    y_copies = [remote(zin.at[3], yin.at[d - 1], y_send.at[d - 1], y_recv.at[d - 1], ys[d - 1]) for d in (1, 2, 3)]
    for cp in y_copies:
        cp.start()
    for k in range(EARLY, PARTS):
        for cc in range(2):
            s_copy(cc, k).start()
    for n in range(len(LAST)):
        for cc in range(2):
            q_copy(cc, n).start()
    for cp in y_copies:
        cp.wait_recv()
    at_z = span(c * n_c + x * n_x + z * n_z, n_z)
    at_x = span(c * n_c + x * n_x, n_x)
    at_c = span(c * n_c, n_c)
    full[at_z, :] = zin[3] + yin[0] + yin[1] + yin[2]

    gz_copies = [remote(full.at[at_z, :], full.at[at_z, :], gz_send.at[d - 1], gz_recv.at[d - 1], zs[d - 1])
                 for d in (1, 2, 3)]
    for cp in gz_copies:
        cp.start()
    for cp in gz_copies:
        cp.wait_recv()
    gx_copies = [remote(full.at[at_x, :], full.at[at_x, :], gx_send.at[d - 1], gx_recv.at[d - 1], xs[d - 1])
                 for d in (1, 2, 3)]
    for cp in gx_copies:
        cp.start()
    for cp in gx_copies:
        cp.wait_recv()
    gc_copy = remote(full.at[at_c, :], full.at[at_c, :], gc_send, gc_recv, sib)
    gc_copy.start()
    gc_copy.wait_recv()

    pair = 2 * rows
    one = spread[:, :1]

    def diagonal(size, row0, col0, axis):
        tile = full[span(row0, size), :] if axis == 1 else full[...]
        r = lax.broadcasted_iota(jnp.int32, tile.shape, 0) + row0
        q = lax.broadcasted_iota(jnp.int32, tile.shape, 1)
        return jnp.sum(jnp.where(r == q, tile, 0.0), axis=axis, keepdims=True)

    own_sq = diagonal(pair, h * pair, 0, 1)
    all_sq = diagonal(count, 0, 0, 0)
    kern = jnp.exp(-(own_sq + all_sq - 2.0 * full[span(h * pair, pair), :]) / one)
    step = jnp.full((1, 128), step_ref[0], jnp.float32)[:, :1]
    gain = step / jnp.float32(count)
    w_ref[...] = jnp.broadcast_to(1.0 + gain * pull * jnp.sum(kern, axis=1, keepdims=True), w_ref.shape)
    kern = gain * kern
    low, high = kern[:, :pair], kern[:, pair:]
    first = h == 0
    k_own[...] = jnp.where(first, low, high)
    k_oth[...] = jnp.where(first, high, low)
    own_rows, oth_rows = span(h * pair, pair), span((1 - h) * pair, pair)

    def product(k_ref, value):
        return jnp.dot(k_ref[...], value, precision=lax.Precision.HIGHEST, preferred_element_type=jnp.float32)

    def of_chip(gi, k):
        particles = pb[gi, own_rows, kcols(k)]
        return w_ref[:, :1] * particles + product(k_own, sb[gi, own_rows, kcols(k)] - pull * particles)

    def first_out(k):
        return remote(ob.at[0, mine(1 - c), kcols(k)], out_ref.at[:, cols(c, h, k, piece)],
                      o_send.at[k], o_recv.at[k], sib)

    def last_out(n):
        where = pl.ds(pl.multiple_of(c * (2 * quarter) + (1 - h) * quarter + unit * sum(LAST[:n]), unit), unit * LAST[n])
        return where, remote(ob.at[1, mine(1 - c), last_at[n]], out_ref.at[:, where],
                             o_send.at[PARTS + n], o_recv.at[PARTS + n], sib)

    sib_copy(1, 0).wait_recv()

    def first_step(k, carry):
        for cc in range(2):
            arrival(sb, 0, cc, k, kcols(k), s_send, s_recv).wait_recv()
        q_oth = sb[0, oth_rows, kcols(k)] - pull * pb[0, oth_rows, kcols(k)]
        ob[0, :, kcols(k)] = of_chip(0, k) + product(k_oth, q_oth)
        first_out(k).start()
        out_ref[:, cols(c, h, k, piece)] = ob[0, mine(c), kcols(k)]
        return carry

    lax.fori_loop(0, PARTS, first_step, 0)
    sib_copy(0, 1).wait_recv()
    sib_copy(1, 1).wait_recv()

    def base_step(k, carry):
        ob[1, :, kcols(k)] = of_chip(1, k)
        return carry

    lax.fori_loop(0, PARTS, base_step, 0)
    for n in range(len(LAST)):
        for cc in range(2):
            arrival(sb, 1, cc, n, last_at[n], q_send, q_recv).wait_recv()
        ob[1, :, last_at[n]] = ob[1, :, last_at[n]] + product(k_oth, sb[1, oth_rows, last_at[n]])
        where, away = last_out(n)
        away.start()
        out_ref[:, where] = ob[1, mine(c), last_at[n]]

    for k in range(PARTS):
        for cc in range(2):
            p_copy(cc, k).wait_send()
            s_copy(cc, k).wait_send()
    for n in range(len(LAST)):
        for cc in range(2):
            q_copy(cc, n).wait_send()
    for n in range(2):
        for gi in range(2):
            sib_copy(n, gi).wait_send()
    copy.wait_send()
    for cp in (*x_copies, *z_copies, *y_copies, *gz_copies, *gx_copies, gc_copy):
        cp.wait_send()
    for k in range(PARTS):
        first_out(k).wait()
    for n in range(len(LAST)):
        last_out(n)[1].wait()


def solution(mesh):
    size_dom = mesh.shape["dom"]

    def on_device(particles, scores, spread, step_size):
        rows, width = particles.shape
        quarter = width // 4
        piece = quarter // PARTS
        count = size_dom * rows
        dma = pltpu.SemaphoreType.DMA
        f32 = jnp.float32
        return pl.pallas_call(
            functools.partial(body, size_dom, rows, quarter),
            out_shape=jax.ShapeDtypeStruct(particles.shape, f32),
            in_specs=[pl.BlockSpec(memory_space=pltpu.SMEM), pl.BlockSpec(memory_space=pltpu.SMEM), pl.BlockSpec(memory_space=pltpu.HBM),
                      pl.BlockSpec(memory_space=pltpu.HBM)],
            out_specs=pl.BlockSpec(memory_space=pltpu.VMEM),
            scratch_shapes=[
                pltpu.VMEM((2, count, quarter), f32),
                pltpu.VMEM((2, count, quarter), f32),
                pltpu.VMEM((2, rows, quarter), f32),
                pltpu.VMEM((2, rows, quarter), f32),
                pltpu.VMEM((2, 2 * rows, quarter), f32),
                pltpu.VMEM((count, count), f32),
                pltpu.VMEM((count // 2, count), f32),
                pltpu.VMEM((4, count // 8, count), f32),
                pltpu.VMEM((4, count // 32, count), f32),
                pltpu.VMEM((3, count // 32, count), f32),
                pltpu.VMEM((count, count), f32),
                pltpu.VMEM((2 * rows, 2 * rows), f32),
                pltpu.VMEM((2 * rows, 2 * rows), f32),
                pltpu.VMEM((2 * rows, 128), f32),
                dma((8,)), dma((2, 2)), dma((2, 2)),
                dma((2, PARTS)), dma((2, PARTS)), dma((2, PARTS)), dma((2, PARTS)),
                dma((2, len(LAST))), dma((2, len(LAST))),
                dma, dma, dma((3,)), dma((3,)), dma((3,)), dma((3,)), dma((3,)), dma((3,)),
                dma((3,)), dma((3,)), dma((3,)), dma((3,)), dma, dma,
                dma((PARTS + len(LAST),)), dma((PARTS + len(LAST),)),
            ],
            compiler_params=pltpu.CompilerParams(
                collective_id=0, has_side_effects=True, vmem_limit_bytes=48 << 20),
            name="svgd",
        )(spread.reshape(1), step_size.reshape(1), particles, scores)

    return jax.shard_map(
        on_device,
        mesh=mesh,
        in_specs=(P("dom", "dim"), P("dom", "dim"), P(), P()),
        out_specs=P("dom", "dim"),
        check_vma=False,
    )
```

```python
import functools

import jax
import jax.numpy as jnp
from jax import lax
from jax.experimental import pallas as pl
from jax.experimental.pallas import tpu as pltpu
from jax.sharding import PartitionSpec as P

MESH = pl.DeviceIdType.MESH
PARTS = 4
EARLY = 3
LAST = (4, 4, 4, 2, 1, 1)


def body(
    size_dom, rows, quarter,
    spread_ref, step_ref, p_ref, s_ref, out_ref,
    pb, sb, pt, qs, ob, gram, half_in, xin, zin, yin, full, k_own, k_oth, w_ref,
    load_sem, sib_send, sib_recv, p_send, p_recv, s_send, s_recv, q_send, q_recv,
    red_send, red_recv, x_send, x_recv, z_send, z_recv, y_send, y_recv,
    gz_send, gz_recv, gx_send, gx_recv, gc_send, gc_recv,
    o_send, o_recv, met,
):
    piece, unit = quarter // PARTS, quarter // 16
    dom, dim = lax.axis_index("dom"), lax.axis_index("dim")
    h, c = dom // 2, lax.rem(dom, 2)
    z, lo, x = dim // 8, lax.rem(dim // 4, 2), lax.rem(dim, 4)
    y = h * 2 + lo
    block = dom

    def dev(hh, cc, zz, ll, xx):
        return (hh * 2 + cc, zz * 8 + ll * 4 + xx)

    sib = dev(h, 1 - c, z, lo, x)
    over = [dev(1 - h, cc, z, lo, x) for cc in range(2)]
    xs = [dev(h, c, z, lo, lax.rem(x + d, 4)) for d in (1, 2, 3)]
    zs = [dev(h, c, lax.rem(z + d, 4), lo, x) for d in (1, 2, 3)]
    ys = []
    for d in (1, 2, 3):
        yy = lax.rem(y + d, 4)
        ys.append(dev(yy // 2, c, z, lax.rem(yy, 2), x))

    barrier = pltpu.get_barrier_semaphore()
    near = [sib, *over]
    wide = [*xs, *zs, ys[0], ys[2]]
    for peer in near:
        pl.semaphore_signal(barrier, inc=1, device_id=peer, device_id_type=MESH)

    @pl.when(c == 0)
    def _():
        for peer in wide:
            pl.semaphore_signal(barrier, inc=1, device_id=peer, device_id_type=MESH)
        pl.semaphore_wait(barrier, len(near) + len(wide))

    @pl.when(c == 1)
    def _():
        pl.semaphore_wait(barrier, len(near))

    def remote(src, dst, ssem, rsem, to):
        return pltpu.make_async_remote_copy(
            src_ref=src, dst_ref=dst, send_sem=ssem, recv_sem=rsem,
            device_id=to, device_id_type=MESH,
        )

    def cols(cc, g, k, width):
        return pl.ds(pl.multiple_of(cc * (2 * quarter) + g * quarter + k * piece, piece), width)

    def mine(b):
        return pl.ds(pl.multiple_of(b * rows, rows), rows)

    def kcols(k):
        return pl.ds(pl.multiple_of(k * piece, piece), piece)

    side = [h, 1 - h]

    def p_copy(cc, k):
        return remote(p_ref.at[:, cols(cc, 1 - h, k, piece)], pb.at[0, mine(block), kcols(k)],
                      p_send.at[cc, k], p_recv.at[c, k], over[cc])

    def s_copy(cc, k):
        return remote(s_ref.at[:, cols(cc, 1 - h, k, piece)], sb.at[0, mine(block), kcols(k)],
                      s_send.at[cc, k], s_recv.at[c, k], over[cc])

    last_at = [pl.ds(unit * sum(LAST[:n]), unit * width) for n, width in enumerate(LAST)]

    def q_copy(cc, n):
        return remote(qs.at[cc, :, last_at[n]], sb.at[1, mine(block), last_at[n]],
                      q_send.at[cc, n], q_recv.at[c, n], over[cc])

    def arrival(buf, gi, cc, k, at, ssem, rsem):
        there = buf.at[gi, mine((1 - h) * 2 + cc), at]
        return remote(there, there, ssem.at[cc, k], rsem.at[cc, k], over[cc])

    def sib_copy(n, gi):
        src, dst = ((p_ref, pb), (s_ref, sb))[n]
        return remote(src.at[:, cols(1 - c, side[gi], 0, quarter)], dst.at[gi, mine(block), :],
                      sib_send.at[n, gi], sib_recv.at[n, gi], sib)

    for k in range(PARTS):
        for cc in range(2):
            p_copy(cc, k).start()
    @pl.when(c == 0)
    def _():
        for peer in wide:
            pl.semaphore_signal(met, inc=1, device_id=peer, device_id_type=MESH)

    loads = []
    for n, (src, dst) in enumerate(((p_ref, pb), (s_ref, sb))):
        for gi in range(2):
            loads.append(pltpu.make_async_copy(
                src.at[:, cols(c, side[gi], 0, quarter)], dst.at[gi, mine(block), :], load_sem.at[2 * n + gi]))
    for cc in range(2):
        loads.append(pltpu.make_async_copy(p_ref.at[:, cols(cc, h, 0, quarter)], pt.at[cc], load_sem.at[4 + cc]))
        loads.append(pltpu.make_async_copy(s_ref.at[:, cols(cc, h, 0, quarter)], qs.at[cc], load_sem.at[6 + cc]))
    for n in range(2):
        for gi in range(2):
            sib_copy(n, gi).start()
    for load in loads:
        load.start()
    for k in range(EARLY):
        for cc in range(2):
            s_copy(cc, k).start()
    for load in loads:
        load.wait()

    spread = jnp.full((1, 128), spread_ref[0], jnp.float32)
    pull = (2.0 / spread)[:, :1]
    for cc in range(2):
        def scale(k, carry, cc=cc):
            qs[cc, :, kcols(k)] = qs[cc, :, kcols(k)] - pull * pt[cc, :, kcols(k)]
            return carry
        lax.fori_loop(0, PARTS, scale, 0)

    sib_copy(0, 0).wait_recv()
    gram[...] = jnp.zeros_like(gram)

    def gram_step(k, carry):
        for cc in range(2):
            arrival(pb, 0, cc, k, kcols(k), p_send, p_recv).wait_recv()
        part = pb[0, :, kcols(k)]
        gram[...] += lax.dot_general(part, part, (((1,), (1,)), ((), ())),
                                     precision=lax.Precision.HIGHEST, preferred_element_type=jnp.float32)
        return carry

    lax.fori_loop(0, PARTS, gram_step, 0)

    count = size_dom * rows
    n_c, n_x, n_z = count // 2, count // 8, count // 32

    def span(start, size):
        return pl.ds(pl.multiple_of(start, size), size)

    @pl.when(c == 0)
    def _():
        pl.semaphore_wait(met, len(wide))
        pl.semaphore_signal(met, inc=1, device_id=sib, device_id_type=MESH)

    @pl.when(c == 1)
    def _():
        pl.semaphore_wait(met, 1)

    copy = remote(gram.at[span((1 - c) * n_c, n_c), :], half_in, red_send, red_recv, sib)
    copy.start()
    copy.wait_recv()
    half_in[...] += gram[span(c * n_c, n_c), :]
    x_copies = [remote(half_in.at[span(lax.rem(x + d, 4) * n_x, n_x), :], xin.at[d - 1],
                       x_send.at[d - 1], x_recv.at[d - 1], xs[d - 1]) for d in (1, 2, 3)]
    for cp in x_copies:
        cp.start()
    for cp in x_copies:
        cp.wait_recv()
    xin[3] = half_in[span(x * n_x, n_x), :] + xin[0] + xin[1] + xin[2]
    z_copies = [remote(xin.at[3, span(lax.rem(z + d, 4) * n_z, n_z), :], zin.at[d - 1],
                       z_send.at[d - 1], z_recv.at[d - 1], zs[d - 1]) for d in (1, 2, 3)]
    for cp in z_copies:
        cp.start()
    for cp in z_copies:
        cp.wait_recv()
    zin[3] = xin[3, span(z * n_z, n_z), :] + zin[0] + zin[1] + zin[2]
    y_copies = [remote(zin.at[3], yin.at[d - 1], y_send.at[d - 1], y_recv.at[d - 1], ys[d - 1]) for d in (1, 2, 3)]
    for cp in y_copies:
        cp.start()
    for k in range(EARLY, PARTS):
        for cc in range(2):
            s_copy(cc, k).start()
    for n in range(len(LAST)):
        for cc in range(2):
            q_copy(cc, n).start()
    for cp in y_copies:
        cp.wait_recv()
    at_z = span(c * n_c + x * n_x + z * n_z, n_z)
    at_x = span(c * n_c + x * n_x, n_x)
    at_c = span(c * n_c, n_c)
    full[at_z, :] = zin[3] + yin[0] + yin[1] + yin[2]

    gz_copies = [remote(full.at[at_z, :], full.at[at_z, :], gz_send.at[d - 1], gz_recv.at[d - 1], zs[d - 1])
                 for d in (1, 2, 3)]
    for cp in gz_copies:
        cp.start()
    for cp in gz_copies:
        cp.wait_recv()
    gx_copies = [remote(full.at[at_x, :], full.at[at_x, :], gx_send.at[d - 1], gx_recv.at[d - 1], xs[d - 1])
                 for d in (1, 2, 3)]
    for cp in gx_copies:
        cp.start()
    for cp in gx_copies:
        cp.wait_recv()
    gc_copy = remote(full.at[at_c, :], full.at[at_c, :], gc_send, gc_recv, sib)
    gc_copy.start()
    gc_copy.wait_recv()

    pair = 2 * rows
    one = spread[:, :1]

    def diagonal(size, row0, col0, axis):
        tile = full[span(row0, size), :] if axis == 1 else full[...]
        r = lax.broadcasted_iota(jnp.int32, tile.shape, 0) + row0
        q = lax.broadcasted_iota(jnp.int32, tile.shape, 1)
        return jnp.sum(jnp.where(r == q, tile, 0.0), axis=axis, keepdims=True)

    own_sq = diagonal(pair, h * pair, 0, 1)
    all_sq = diagonal(count, 0, 0, 0)
    kern = jnp.exp(-(own_sq + all_sq - 2.0 * full[span(h * pair, pair), :]) / one)
    step = jnp.full((1, 128), step_ref[0], jnp.float32)[:, :1]
    gain = step / jnp.float32(count)
    w_ref[...] = jnp.broadcast_to(1.0 + gain * pull * jnp.sum(kern, axis=1, keepdims=True), w_ref.shape)
    kern = gain * kern
    low, high = kern[:, :pair], kern[:, pair:]
    first = h == 0
    k_own[...] = jnp.where(first, low, high)
    k_oth[...] = jnp.where(first, high, low)
    own_rows, oth_rows = span(h * pair, pair), span((1 - h) * pair, pair)

    def product(k_ref, value):
        return jnp.dot(k_ref[...], value, precision=lax.Precision.HIGHEST, preferred_element_type=jnp.float32)

    def of_chip(gi, k):
        particles = pb[gi, own_rows, kcols(k)]
        return w_ref[:, :1] * particles + product(k_own, sb[gi, own_rows, kcols(k)] - pull * particles)

    def first_out(k):
        return remote(ob.at[0, mine(1 - c), kcols(k)], out_ref.at[:, cols(c, h, k, piece)],
                      o_send.at[k], o_recv.at[k], sib)

    def last_out(n):
        where = pl.ds(pl.multiple_of(c * (2 * quarter) + (1 - h) * quarter + unit * sum(LAST[:n]), unit), unit * LAST[n])
        return where, remote(ob.at[1, mine(1 - c), last_at[n]], out_ref.at[:, where],
                             o_send.at[PARTS + n], o_recv.at[PARTS + n], sib)

    sib_copy(1, 0).wait_recv()

    def first_step(k, carry):
        for cc in range(2):
            arrival(sb, 0, cc, k, kcols(k), s_send, s_recv).wait_recv()
        q_oth = sb[0, oth_rows, kcols(k)] - pull * pb[0, oth_rows, kcols(k)]
        ob[0, :, kcols(k)] = of_chip(0, k) + product(k_oth, q_oth)
        first_out(k).start()
        out_ref[:, cols(c, h, k, piece)] = ob[0, mine(c), kcols(k)]
        return carry

    lax.fori_loop(0, PARTS, first_step, 0)
    sib_copy(0, 1).wait_recv()
    sib_copy(1, 1).wait_recv()

    def base_step(k, carry):
        ob[1, :, kcols(k)] = of_chip(1, k)
        return carry

    lax.fori_loop(0, PARTS, base_step, 0)
    for n in range(len(LAST)):
        for cc in range(2):
            arrival(sb, 1, cc, n, last_at[n], q_send, q_recv).wait_recv()
        ob[1, :, last_at[n]] = ob[1, :, last_at[n]] + product(k_oth, sb[1, oth_rows, last_at[n]])
        where, away = last_out(n)
        away.start()
        out_ref[:, where] = ob[1, mine(c), last_at[n]]

    for k in range(PARTS):
        for cc in range(2):
            p_copy(cc, k).wait_send()
            s_copy(cc, k).wait_send()
    for n in range(len(LAST)):
        for cc in range(2):
            q_copy(cc, n).wait_send()
    for n in range(2):
        for gi in range(2):
            sib_copy(n, gi).wait_send()
    copy.wait_send()
    for cp in (*x_copies, *z_copies, *y_copies, *gz_copies, *gx_copies, gc_copy):
        cp.wait_send()
    for k in range(PARTS):
        first_out(k).wait()
    for n in range(len(LAST)):
        last_out(n)[1].wait()


def solution(mesh):
    size_dom = mesh.shape["dom"]

    def on_device(particles, scores, spread, step_size):
        rows, width = particles.shape
        quarter = width // 4
        piece = quarter // PARTS
        count = size_dom * rows
        dma = pltpu.SemaphoreType.DMA
        f32 = jnp.float32
        return pl.pallas_call(
            functools.partial(body, size_dom, rows, quarter),
            out_shape=jax.ShapeDtypeStruct(particles.shape, f32),
            in_specs=[pl.BlockSpec(memory_space=pltpu.SMEM), pl.BlockSpec(memory_space=pltpu.SMEM), pl.BlockSpec(memory_space=pltpu.HBM),
                      pl.BlockSpec(memory_space=pltpu.HBM)],
            out_specs=pl.BlockSpec(memory_space=pltpu.VMEM),
            scratch_shapes=[
                pltpu.VMEM((2, count, quarter), f32),
                pltpu.VMEM((2, count, quarter), f32),
                pltpu.VMEM((2, rows, quarter), f32),
                pltpu.VMEM((2, rows, quarter), f32),
                pltpu.VMEM((2, 2 * rows, quarter), f32),
                pltpu.VMEM((count, count), f32),
                pltpu.VMEM((count // 2, count), f32),
                pltpu.VMEM((4, count // 8, count), f32),
                pltpu.VMEM((4, count // 32, count), f32),
                pltpu.VMEM((3, count // 32, count), f32),
                pltpu.VMEM((count, count), f32),
                pltpu.VMEM((2 * rows, 2 * rows), f32),
                pltpu.VMEM((2 * rows, 2 * rows), f32),
                pltpu.VMEM((2 * rows, 128), f32),
                dma((8,)), dma((2, 2)), dma((2, 2)),
                dma((2, PARTS)), dma((2, PARTS)), dma((2, PARTS)), dma((2, PARTS)),
                dma((2, len(LAST))), dma((2, len(LAST))),
                dma, dma, dma((3,)), dma((3,)), dma((3,)), dma((3,)), dma((3,)), dma((3,)),
                dma((3,)), dma((3,)), dma((3,)), dma((3,)), dma, dma,
                dma((PARTS + len(LAST),)), dma((PARTS + len(LAST),)),
                pltpu.SemaphoreType.REGULAR,
            ],
            compiler_params=pltpu.CompilerParams(
                collective_id=0, has_side_effects=True, vmem_limit_bytes=48 << 20),
            name="svgd",
        )(spread.reshape(1), step_size.reshape(1), particles, scores)

    return jax.shard_map(
        on_device,
        mesh=mesh,
        in_specs=(P("dom", "dim"), P("dom", "dim"), P(), P()),
        out_specs=P("dom", "dim"),
        check_vma=False,
    )
```

```python
import functools

import jax
import jax.numpy as jnp
from jax import lax
from jax.experimental import pallas as pl
from jax.experimental.pallas import tpu as pltpu
from jax.sharding import PartitionSpec as P

MESH = pl.DeviceIdType.MESH
PARTS = 4
EARLY = 3
LAST = (4, 4, 4, 2, 1, 1)


def body(
    size_dom, rows, quarter,
    spread_ref, step_ref, p_ref, s_ref, out_ref,
    pb, sb, pt, qs, first, ob, gram, half_in, xin, zin, yin, full, k_own, k_oth, w_ref,
    load_sem, sib_send, sib_recv, p_send, p_recv, s_send, s_recv, q_send, q_recv,
    red_send, red_recv, x_send, x_recv, z_send, z_recv, y_send, y_recv,
    gz_send, gz_recv, gx_send, gx_recv, gc_send, gc_recv,
    o_send, o_recv, met,
):
    piece, unit = quarter // PARTS, quarter // 16
    dom, dim = lax.axis_index("dom"), lax.axis_index("dim")
    h, c = dom // 2, lax.rem(dom, 2)
    z, lo, x = dim // 8, lax.rem(dim // 4, 2), lax.rem(dim, 4)
    y = h * 2 + lo
    block = dom

    def dev(hh, cc, zz, ll, xx):
        return (hh * 2 + cc, zz * 8 + ll * 4 + xx)

    sib = dev(h, 1 - c, z, lo, x)
    over = [dev(1 - h, cc, z, lo, x) for cc in range(2)]
    xs = [dev(h, c, z, lo, lax.rem(x + d, 4)) for d in (1, 2, 3)]
    zs = [dev(h, c, lax.rem(z + d, 4), lo, x) for d in (1, 2, 3)]
    ys = []
    for d in (1, 2, 3):
        yy = lax.rem(y + d, 4)
        ys.append(dev(yy // 2, c, z, lax.rem(yy, 2), x))

    ahead = [pltpu.make_async_copy(p_ref.at[:, pl.ds(pl.multiple_of(cc * (2 * quarter) + (1 - h) * quarter, piece), piece)],
                                   first.at[cc], load_sem.at[8 + cc]) for cc in range(2)]
    for load in ahead:
        load.start()

    barrier = pltpu.get_barrier_semaphore()
    near = [sib, *over]
    wide = [*xs, *zs, ys[0], ys[2]]
    for peer in near:
        pl.semaphore_signal(barrier, inc=1, device_id=peer, device_id_type=MESH)

    @pl.when(c == 0)
    def _():
        for peer in wide:
            pl.semaphore_signal(barrier, inc=1, device_id=peer, device_id_type=MESH)
        pl.semaphore_wait(barrier, len(near) + len(wide))

    @pl.when(c == 1)
    def _():
        pl.semaphore_wait(barrier, len(near))

    def remote(src, dst, ssem, rsem, to):
        return pltpu.make_async_remote_copy(
            src_ref=src, dst_ref=dst, send_sem=ssem, recv_sem=rsem,
            device_id=to, device_id_type=MESH,
        )

    def cols(cc, g, k, width):
        return pl.ds(pl.multiple_of(cc * (2 * quarter) + g * quarter + k * piece, piece), width)

    def mine(b):
        return pl.ds(pl.multiple_of(b * rows, rows), rows)

    def kcols(k):
        return pl.ds(pl.multiple_of(k * piece, piece), piece)

    side = [h, 1 - h]

    def p_copy(cc, k):
        source = first.at[cc] if k == 0 else p_ref.at[:, cols(cc, 1 - h, k, piece)]
        return remote(source, pb.at[0, mine(block), kcols(k)],
                      p_send.at[cc, k], p_recv.at[c, k], over[cc])

    def s_copy(cc, k):
        return remote(s_ref.at[:, cols(cc, 1 - h, k, piece)], sb.at[0, mine(block), kcols(k)],
                      s_send.at[cc, k], s_recv.at[c, k], over[cc])

    last_at = [pl.ds(unit * sum(LAST[:n]), unit * width) for n, width in enumerate(LAST)]

    def q_copy(cc, n):
        return remote(qs.at[cc, :, last_at[n]], sb.at[1, mine(block), last_at[n]],
                      q_send.at[cc, n], q_recv.at[c, n], over[cc])

    def arrival(buf, gi, cc, k, at, ssem, rsem):
        there = buf.at[gi, mine((1 - h) * 2 + cc), at]
        return remote(there, there, ssem.at[cc, k], rsem.at[cc, k], over[cc])

    def sib_copy(n, gi):
        src, dst = ((p_ref, pb), (s_ref, sb))[n]
        return remote(src.at[:, cols(1 - c, side[gi], 0, quarter)], dst.at[gi, mine(block), :],
                      sib_send.at[n, gi], sib_recv.at[n, gi], sib)

    for k in range(PARTS):
        for cc in range(2):
            if k == 0:
                ahead[cc].wait()
            p_copy(cc, k).start()
    @pl.when(c == 0)
    def _():
        for peer in wide:
            pl.semaphore_signal(met, inc=1, device_id=peer, device_id_type=MESH)

    loads = []
    for n, (src, dst) in enumerate(((p_ref, pb), (s_ref, sb))):
        for gi in range(2):
            loads.append(pltpu.make_async_copy(
                src.at[:, cols(c, side[gi], 0, quarter)], dst.at[gi, mine(block), :], load_sem.at[2 * n + gi]))
    for cc in range(2):
        loads.append(pltpu.make_async_copy(p_ref.at[:, cols(cc, h, 0, quarter)], pt.at[cc], load_sem.at[4 + cc]))
        loads.append(pltpu.make_async_copy(s_ref.at[:, cols(cc, h, 0, quarter)], qs.at[cc], load_sem.at[6 + cc]))
    for n in range(2):
        for gi in range(2):
            sib_copy(n, gi).start()
    for load in loads:
        load.start()
    for k in range(EARLY):
        for cc in range(2):
            s_copy(cc, k).start()
    for load in loads:
        load.wait()

    spread = jnp.full((1, 128), spread_ref[0], jnp.float32)
    pull = (2.0 / spread)[:, :1]
    for cc in range(2):
        def scale(k, carry, cc=cc):
            qs[cc, :, kcols(k)] = qs[cc, :, kcols(k)] - pull * pt[cc, :, kcols(k)]
            return carry
        lax.fori_loop(0, PARTS, scale, 0)

    sib_copy(0, 0).wait_recv()
    gram[...] = jnp.zeros_like(gram)

    def gram_step(k, carry):
        for cc in range(2):
            arrival(pb, 0, cc, k, kcols(k), p_send, p_recv).wait_recv()
        part = pb[0, :, kcols(k)]
        gram[...] += lax.dot_general(part, part, (((1,), (1,)), ((), ())),
                                     precision=lax.Precision.HIGHEST, preferred_element_type=jnp.float32)
        return carry

    lax.fori_loop(0, PARTS, gram_step, 0)

    count = size_dom * rows
    n_c, n_x, n_z = count // 2, count // 8, count // 32

    def span(start, size):
        return pl.ds(pl.multiple_of(start, size), size)

    @pl.when(c == 0)
    def _():
        pl.semaphore_wait(met, len(wide))
        pl.semaphore_signal(met, inc=1, device_id=sib, device_id_type=MESH)

    @pl.when(c == 1)
    def _():
        pl.semaphore_wait(met, 1)

    copy = remote(gram.at[span((1 - c) * n_c, n_c), :], half_in, red_send, red_recv, sib)
    copy.start()
    copy.wait_recv()
    half_in[...] += gram[span(c * n_c, n_c), :]
    x_copies = [remote(half_in.at[span(lax.rem(x + d, 4) * n_x, n_x), :], xin.at[d - 1],
                       x_send.at[d - 1], x_recv.at[d - 1], xs[d - 1]) for d in (1, 2, 3)]
    for cp in x_copies:
        cp.start()
    for cp in x_copies:
        cp.wait_recv()
    xin[3] = half_in[span(x * n_x, n_x), :] + xin[0] + xin[1] + xin[2]
    z_copies = [remote(xin.at[3, span(lax.rem(z + d, 4) * n_z, n_z), :], zin.at[d - 1],
                       z_send.at[d - 1], z_recv.at[d - 1], zs[d - 1]) for d in (1, 2, 3)]
    for cp in z_copies:
        cp.start()
    for cp in z_copies:
        cp.wait_recv()
    zin[3] = xin[3, span(z * n_z, n_z), :] + zin[0] + zin[1] + zin[2]
    tile = pl.ds(pl.multiple_of((c * 2 + x // 2) * 128, 128), 128)

    def y_copy(d, whole):
        src, dst = zin.at[3], yin.at[d - 1]
        if not whole:
            src, dst = src.at[:, tile], dst.at[:, tile]
        return remote(src, dst, y_send.at[d - 1], y_recv.at[d - 1], ys[d - 1])

    def on_y(act, of):
        for d in (1, 2, 3):
            use = of(d)

            @pl.when(use == c)
            def _(d=d):
                act(y_copy(d, True))

            @pl.when(use != c)
            def _(d=d):
                act(y_copy(d, False))

    def receiver(d):
        return lax.rem(y + d, 4) // 2

    on_y(lambda cp: cp.start(), receiver)
    for k in range(EARLY, PARTS):
        for cc in range(2):
            s_copy(cc, k).start()
    for n in range(len(LAST)):
        for cc in range(2):
            q_copy(cc, n).start()
    on_y(lambda cp: cp.wait_recv(), lambda d: h)
    at_z = span(c * n_c + x * n_x + z * n_z, n_z)
    at_x = span(c * n_c + x * n_x, n_x)
    at_c = span(c * n_c, n_c)

    @pl.when(h == c)
    def _():
        full[at_z, :] = zin[3] + yin[0] + yin[1] + yin[2]

    @pl.when(h != c)
    def _():
        full[at_z, :] = zin[3]
        full[at_z, tile] = zin[3, :, tile] + yin[0, :, tile] + yin[1, :, tile] + yin[2, :, tile]

    gz_copies = [remote(full.at[at_z, :], full.at[at_z, :], gz_send.at[d - 1], gz_recv.at[d - 1], zs[d - 1])
                 for d in (1, 2, 3)]
    for cp in gz_copies:
        cp.start()
    for cp in gz_copies:
        cp.wait_recv()
    gx_copies = [remote(full.at[at_x, :], full.at[at_x, :], gx_send.at[d - 1], gx_recv.at[d - 1], xs[d - 1])
                 for d in (1, 2, 3)]
    for cp in gx_copies:
        cp.start()
    for cp in gx_copies:
        cp.wait_recv()
    gc_copy = remote(full.at[at_c, :], full.at[at_c, :], gc_send, gc_recv, sib)
    gc_copy.start()
    gc_copy.wait_recv()

    pair = 2 * rows
    one = spread[:, :1]

    def diagonal(size, row0, col0, axis):
        tile = full[span(row0, size), :] if axis == 1 else full[...]
        r = lax.broadcasted_iota(jnp.int32, tile.shape, 0) + row0
        q = lax.broadcasted_iota(jnp.int32, tile.shape, 1)
        return jnp.sum(jnp.where(r == q, tile, 0.0), axis=axis, keepdims=True)

    own_sq = diagonal(pair, h * pair, 0, 1)
    all_sq = diagonal(count, 0, 0, 0)
    kern = jnp.exp(-(own_sq + all_sq - 2.0 * full[span(h * pair, pair), :]) / one)
    step = jnp.full((1, 128), step_ref[0], jnp.float32)[:, :1]
    gain = step / jnp.float32(count)
    w_ref[...] = jnp.broadcast_to(1.0 + gain * pull * jnp.sum(kern, axis=1, keepdims=True), w_ref.shape)
    kern = gain * kern
    low, high = kern[:, :pair], kern[:, pair:]
    upper = h == 0
    k_own[...] = jnp.where(upper, low, high)
    k_oth[...] = jnp.where(upper, high, low)
    own_rows, oth_rows = span(h * pair, pair), span((1 - h) * pair, pair)

    def product(k_ref, value):
        return jnp.dot(k_ref[...], value, precision=lax.Precision.HIGHEST, preferred_element_type=jnp.float32)

    def of_chip(gi, k):
        particles = pb[gi, own_rows, kcols(k)]
        return w_ref[:, :1] * particles + product(k_own, sb[gi, own_rows, kcols(k)] - pull * particles)

    def first_out(k):
        return remote(ob.at[0, mine(1 - c), kcols(k)], out_ref.at[:, cols(c, h, k, piece)],
                      o_send.at[k], o_recv.at[k], sib)

    def last_out(n):
        where = pl.ds(pl.multiple_of(c * (2 * quarter) + (1 - h) * quarter + unit * sum(LAST[:n]), unit), unit * LAST[n])
        return where, remote(ob.at[1, mine(1 - c), last_at[n]], out_ref.at[:, where],
                             o_send.at[PARTS + n], o_recv.at[PARTS + n], sib)

    sib_copy(1, 0).wait_recv()

    def first_step(k, carry):
        for cc in range(2):
            arrival(sb, 0, cc, k, kcols(k), s_send, s_recv).wait_recv()
        q_oth = sb[0, oth_rows, kcols(k)] - pull * pb[0, oth_rows, kcols(k)]
        ob[0, :, kcols(k)] = of_chip(0, k) + product(k_oth, q_oth)
        first_out(k).start()
        out_ref[:, cols(c, h, k, piece)] = ob[0, mine(c), kcols(k)]
        return carry

    lax.fori_loop(0, PARTS, first_step, 0)
    sib_copy(0, 1).wait_recv()
    sib_copy(1, 1).wait_recv()

    def base_step(k, carry):
        ob[1, :, kcols(k)] = of_chip(1, k)
        return carry

    lax.fori_loop(0, PARTS, base_step, 0)
    for n in range(len(LAST)):
        for cc in range(2):
            arrival(sb, 1, cc, n, last_at[n], q_send, q_recv).wait_recv()
        q_oth = sb[1, oth_rows, last_at[n]]
        where, away = last_out(n)
        ob[1, mine(1 - c), last_at[n]] = ob[1, mine(1 - c), last_at[n]] + product(k_oth.at[mine(1 - c), :], q_oth)
        away.start()
        out_ref[:, where] = ob[1, mine(c), last_at[n]] + product(k_oth.at[mine(c), :], q_oth)

    for k in range(PARTS):
        for cc in range(2):
            p_copy(cc, k).wait_send()
            s_copy(cc, k).wait_send()
    for n in range(len(LAST)):
        for cc in range(2):
            q_copy(cc, n).wait_send()
    for n in range(2):
        for gi in range(2):
            sib_copy(n, gi).wait_send()
    copy.wait_send()
    on_y(lambda cp: cp.wait_send(), receiver)
    for cp in (*x_copies, *z_copies, *gz_copies, *gx_copies, gc_copy):
        cp.wait_send()
    for k in range(PARTS):
        first_out(k).wait()
    for n in range(len(LAST)):
        last_out(n)[1].wait()


def solution(mesh):
    size_dom = mesh.shape["dom"]

    def on_device(particles, scores, spread, step_size):
        rows, width = particles.shape
        quarter = width // 4
        piece = quarter // PARTS
        count = size_dom * rows
        dma = pltpu.SemaphoreType.DMA
        f32 = jnp.float32
        return pl.pallas_call(
            functools.partial(body, size_dom, rows, quarter),
            out_shape=jax.ShapeDtypeStruct(particles.shape, f32),
            in_specs=[pl.BlockSpec(memory_space=pltpu.SMEM), pl.BlockSpec(memory_space=pltpu.SMEM), pl.BlockSpec(memory_space=pltpu.HBM),
                      pl.BlockSpec(memory_space=pltpu.HBM)],
            out_specs=pl.BlockSpec(memory_space=pltpu.VMEM),
            scratch_shapes=[
                pltpu.VMEM((2, count, quarter), f32),
                pltpu.VMEM((2, count, quarter), f32),
                pltpu.VMEM((2, rows, quarter), f32),
                pltpu.VMEM((2, rows, quarter), f32),
                pltpu.VMEM((2, rows, piece), f32),
                pltpu.VMEM((2, 2 * rows, quarter), f32),
                pltpu.VMEM((count, count), f32),
                pltpu.VMEM((count // 2, count), f32),
                pltpu.VMEM((4, count // 8, count), f32),
                pltpu.VMEM((4, count // 32, count), f32),
                pltpu.VMEM((3, count // 32, count), f32),
                pltpu.VMEM((count, count), f32),
                pltpu.VMEM((2 * rows, 2 * rows), f32),
                pltpu.VMEM((2 * rows, 2 * rows), f32),
                pltpu.VMEM((2 * rows, 128), f32),
                dma((10,)), dma((2, 2)), dma((2, 2)),
                dma((2, PARTS)), dma((2, PARTS)), dma((2, PARTS)), dma((2, PARTS)),
                dma((2, len(LAST))), dma((2, len(LAST))),
                dma, dma, dma((3,)), dma((3,)), dma((3,)), dma((3,)), dma((3,)), dma((3,)),
                dma((3,)), dma((3,)), dma((3,)), dma((3,)), dma, dma,
                dma((PARTS + len(LAST),)), dma((PARTS + len(LAST),)),
                pltpu.SemaphoreType.REGULAR,
            ],
            compiler_params=pltpu.CompilerParams(
                collective_id=0, has_side_effects=True, vmem_limit_bytes=48 << 20),
            name="svgd",
        )(spread.reshape(1), step_size.reshape(1), particles, scores)

    return jax.shard_map(
        on_device,
        mesh=mesh,
        in_specs=(P("dom", "dim"), P("dom", "dim"), P(), P()),
        out_specs=P("dom", "dim"),
        check_vma=False,
    )
```

```python
import functools

import jax
import jax.numpy as jnp
from jax import lax
from jax.experimental import pallas as pl
from jax.experimental.pallas import tpu as pltpu
from jax.sharding import PartitionSpec as P

MESH = pl.DeviceIdType.MESH
PARTS = 2
EARLY = 2
LAST = (8, 4, 2, 1, 1)


def body(
    size_dom, rows, quarter,
    spread_ref, step_ref, p_ref, s_ref, out_ref,
    pb, sb, pt, qs, first, ob, gram, half_in, xin, zin, yin, full, k_own, k_oth, w_ref,
    load_sem, sib_send, sib_recv, p_send, p_recv, s_send, s_recv, q_send, q_recv,
    red_send, red_recv, x_send, x_recv, z_send, z_recv, y_send, y_recv,
    gz_send, gz_recv, gx_send, gx_recv, gc_send, gc_recv,
    o_send, o_recv, met,
):
    piece, unit = quarter // PARTS, quarter // 16
    dom, dim = lax.axis_index("dom"), lax.axis_index("dim")
    h, c = dom // 2, lax.rem(dom, 2)
    z, lo, x = dim // 8, lax.rem(dim // 4, 2), lax.rem(dim, 4)
    y = h * 2 + lo
    block = dom

    def dev(hh, cc, zz, ll, xx):
        return (hh * 2 + cc, zz * 8 + ll * 4 + xx)

    sib = dev(h, 1 - c, z, lo, x)
    over = [dev(1 - h, cc, z, lo, x) for cc in range(2)]
    xs = [dev(h, c, z, lo, lax.rem(x + d, 4)) for d in (1, 2, 3)]
    zs = [dev(h, c, lax.rem(z + d, 4), lo, x) for d in (1, 2, 3)]
    ys = []
    for d in (1, 2, 3):
        yy = lax.rem(y + d, 4)
        ys.append(dev(yy // 2, c, z, lax.rem(yy, 2), x))

    ahead = [pltpu.make_async_copy(p_ref.at[:, pl.ds(pl.multiple_of(cc * (2 * quarter) + (1 - h) * quarter, piece), piece)],
                                   first.at[cc], load_sem.at[8 + cc]) for cc in range(2)]
    for load in ahead:
        load.start()

    barrier = pltpu.get_barrier_semaphore()
    near = [sib, *over]
    wide = [*xs, *zs, ys[0], ys[2]]
    for peer in near:
        pl.semaphore_signal(barrier, inc=1, device_id=peer, device_id_type=MESH)

    @pl.when(c == 0)
    def _():
        for peer in wide:
            pl.semaphore_signal(barrier, inc=1, device_id=peer, device_id_type=MESH)
        pl.semaphore_wait(barrier, len(near) + len(wide))

    @pl.when(c == 1)
    def _():
        pl.semaphore_wait(barrier, len(near))

    def remote(src, dst, ssem, rsem, to):
        return pltpu.make_async_remote_copy(
            src_ref=src, dst_ref=dst, send_sem=ssem, recv_sem=rsem,
            device_id=to, device_id_type=MESH,
        )

    def cols(cc, g, k, width):
        return pl.ds(pl.multiple_of(cc * (2 * quarter) + g * quarter + k * piece, piece), width)

    def mine(b):
        return pl.ds(pl.multiple_of(b * rows, rows), rows)

    def kcols(k):
        return pl.ds(pl.multiple_of(k * piece, piece), piece)

    side = [h, 1 - h]

    def p_copy(cc, k):
        source = first.at[cc] if k == 0 else p_ref.at[:, cols(cc, 1 - h, k, piece)]
        return remote(source, pb.at[0, mine(block), kcols(k)],
                      p_send.at[cc, k], p_recv.at[c, k], over[cc])

    def s_copy(cc, k):
        return remote(s_ref.at[:, cols(cc, 1 - h, k, piece)], sb.at[0, mine(block), kcols(k)],
                      s_send.at[cc, k], s_recv.at[c, k], over[cc])

    last_at = [pl.ds(unit * sum(LAST[:n]), unit * width) for n, width in enumerate(LAST)]

    def q_copy(cc, n):
        return remote(qs.at[cc, :, last_at[n]], sb.at[1, mine(block), last_at[n]],
                      q_send.at[cc, n], q_recv.at[c, n], over[cc])

    def arrival(buf, gi, cc, k, at, ssem, rsem):
        there = buf.at[gi, mine((1 - h) * 2 + cc), at]
        return remote(there, there, ssem.at[cc, k], rsem.at[cc, k], over[cc])

    def sib_copy(n, gi):
        src, dst = ((p_ref, pb), (s_ref, sb))[n]
        return remote(src.at[:, cols(1 - c, side[gi], 0, quarter)], dst.at[gi, mine(block), :],
                      sib_send.at[n, gi], sib_recv.at[n, gi], sib)

    for k in range(PARTS):
        for cc in range(2):
            if k == 0:
                ahead[cc].wait()
            p_copy(cc, k).start()
    @pl.when(c == 0)
    def _():
        for peer in wide:
            pl.semaphore_signal(met, inc=1, device_id=peer, device_id_type=MESH)

    loads = []
    for n, (src, dst) in enumerate(((p_ref, pb), (s_ref, sb))):
        for gi in range(2):
            loads.append(pltpu.make_async_copy(
                src.at[:, cols(c, side[gi], 0, quarter)], dst.at[gi, mine(block), :], load_sem.at[2 * n + gi]))
    for cc in range(2):
        loads.append(pltpu.make_async_copy(p_ref.at[:, cols(cc, h, 0, quarter)], pt.at[cc], load_sem.at[4 + cc]))
        loads.append(pltpu.make_async_copy(s_ref.at[:, cols(cc, h, 0, quarter)], qs.at[cc], load_sem.at[6 + cc]))
    for n in range(2):
        for gi in range(2):
            sib_copy(n, gi).start()
    for load in loads:
        load.start()
    for k in range(EARLY):
        for cc in range(2):
            s_copy(cc, k).start()
    for load in loads:
        load.wait()

    spread = jnp.full((1, 128), spread_ref[0], jnp.float32)
    pull = (2.0 / spread)[:, :1]
    for cc in range(2):
        def scale(k, carry, cc=cc):
            qs[cc, :, kcols(k)] = qs[cc, :, kcols(k)] - pull * pt[cc, :, kcols(k)]
            return carry
        lax.fori_loop(0, PARTS, scale, 0)

    sib_copy(0, 0).wait_recv()
    gram[...] = jnp.zeros_like(gram)

    def gram_step(k, carry):
        for cc in range(2):
            arrival(pb, 0, cc, k, kcols(k), p_send, p_recv).wait_recv()
        part = pb[0, :, kcols(k)]
        gram[...] += lax.dot_general(part, part, (((1,), (1,)), ((), ())),
                                     precision=lax.Precision.HIGHEST, preferred_element_type=jnp.float32)
        return carry

    lax.fori_loop(0, PARTS, gram_step, 0)

    count = size_dom * rows
    n_c, n_x, n_z = count // 2, count // 8, count // 32

    def span(start, size):
        return pl.ds(pl.multiple_of(start, size), size)

    @pl.when(c == 0)
    def _():
        pl.semaphore_wait(met, len(wide))
        pl.semaphore_signal(met, inc=1, device_id=sib, device_id_type=MESH)

    @pl.when(c == 1)
    def _():
        pl.semaphore_wait(met, 1)

    copy = remote(gram.at[span((1 - c) * n_c, n_c), :], half_in, red_send, red_recv, sib)
    copy.start()
    copy.wait_recv()
    half_in[...] += gram[span(c * n_c, n_c), :]
    x_copies = [remote(half_in.at[span(lax.rem(x + d, 4) * n_x, n_x), :], xin.at[d - 1],
                       x_send.at[d - 1], x_recv.at[d - 1], xs[d - 1]) for d in (1, 2, 3)]
    for cp in x_copies:
        cp.start()
    for cp in x_copies:
        cp.wait_recv()
    xin[3] = half_in[span(x * n_x, n_x), :] + xin[0] + xin[1] + xin[2]
    z_copies = [remote(xin.at[3, span(lax.rem(z + d, 4) * n_z, n_z), :], zin.at[d - 1],
                       z_send.at[d - 1], z_recv.at[d - 1], zs[d - 1]) for d in (1, 2, 3)]
    for cp in z_copies:
        cp.start()
    for cp in z_copies:
        cp.wait_recv()
    zin[3] = xin[3, span(z * n_z, n_z), :] + zin[0] + zin[1] + zin[2]
    tile = pl.ds(pl.multiple_of((c * 2 + x // 2) * 128, 128), 128)

    def y_copy(d, whole):
        src, dst = zin.at[3], yin.at[d - 1]
        if not whole:
            src, dst = src.at[:, tile], dst.at[:, tile]
        return remote(src, dst, y_send.at[d - 1], y_recv.at[d - 1], ys[d - 1])

    def on_y(act, of):
        for d in (1, 2, 3):
            use = of(d)

            @pl.when(use == c)
            def _(d=d):
                act(y_copy(d, True))

            @pl.when(use != c)
            def _(d=d):
                act(y_copy(d, False))

    def receiver(d):
        return lax.rem(y + d, 4) // 2

    on_y(lambda cp: cp.start(), receiver)
    for k in range(EARLY, PARTS):
        for cc in range(2):
            s_copy(cc, k).start()
    for n in range(len(LAST)):
        for cc in range(2):
            q_copy(cc, n).start()
    on_y(lambda cp: cp.wait_recv(), lambda d: h)
    at_z = span(c * n_c + x * n_x + z * n_z, n_z)
    at_x = span(c * n_c + x * n_x, n_x)
    at_c = span(c * n_c, n_c)

    @pl.when(h == c)
    def _():
        full[at_z, :] = zin[3] + yin[0] + yin[1] + yin[2]

    @pl.when(h != c)
    def _():
        full[at_z, :] = zin[3]
        full[at_z, tile] = zin[3, :, tile] + yin[0, :, tile] + yin[1, :, tile] + yin[2, :, tile]

    gz_copies = [remote(full.at[at_z, :], full.at[at_z, :], gz_send.at[d - 1], gz_recv.at[d - 1], zs[d - 1])
                 for d in (1, 2, 3)]
    for cp in gz_copies:
        cp.start()
    for cp in gz_copies:
        cp.wait_recv()
    gx_copies = [remote(full.at[at_x, :], full.at[at_x, :], gx_send.at[d - 1], gx_recv.at[d - 1], xs[d - 1])
                 for d in (1, 2, 3)]
    for cp in gx_copies:
        cp.start()
    for cp in gx_copies:
        cp.wait_recv()
    gc_copy = remote(full.at[at_c, :], full.at[at_c, :], gc_send, gc_recv, sib)
    gc_copy.start()
    gc_copy.wait_recv()

    pair = 2 * rows
    one = spread[:, :1]

    def diagonal(size, row0, col0, axis):
        tile = full[span(row0, size), :] if axis == 1 else full[...]
        r = lax.broadcasted_iota(jnp.int32, tile.shape, 0) + row0
        q = lax.broadcasted_iota(jnp.int32, tile.shape, 1)
        return jnp.sum(jnp.where(r == q, tile, 0.0), axis=axis, keepdims=True)

    own_sq = diagonal(pair, h * pair, 0, 1)
    all_sq = diagonal(count, 0, 0, 0)
    kern = jnp.exp(-(own_sq + all_sq - 2.0 * full[span(h * pair, pair), :]) / one)
    step = jnp.full((1, 128), step_ref[0], jnp.float32)[:, :1]
    gain = step / jnp.float32(count)
    w_ref[...] = jnp.broadcast_to(1.0 + gain * pull * jnp.sum(kern, axis=1, keepdims=True), w_ref.shape)
    kern = gain * kern
    low, high = kern[:, :pair], kern[:, pair:]
    upper = h == 0
    k_own[...] = jnp.where(upper, low, high)
    k_oth[...] = jnp.where(upper, high, low)
    own_rows, oth_rows = span(h * pair, pair), span((1 - h) * pair, pair)

    def product(k_ref, value):
        return jnp.dot(k_ref[...], value, precision=lax.Precision.HIGHEST, preferred_element_type=jnp.float32)

    def of_chip(gi, k):
        particles = pb[gi, own_rows, kcols(k)]
        return w_ref[:, :1] * particles + product(k_own, sb[gi, own_rows, kcols(k)] - pull * particles)

    def first_out(k):
        return remote(ob.at[0, mine(1 - c), kcols(k)], out_ref.at[:, cols(c, h, k, piece)],
                      o_send.at[k], o_recv.at[k], sib)

    def last_out(n):
        where = pl.ds(pl.multiple_of(c * (2 * quarter) + (1 - h) * quarter + unit * sum(LAST[:n]), unit), unit * LAST[n])
        return where, remote(ob.at[1, mine(1 - c), last_at[n]], out_ref.at[:, where],
                             o_send.at[PARTS + n], o_recv.at[PARTS + n], sib)

    sib_copy(1, 0).wait_recv()

    def first_step(k, carry):
        for cc in range(2):
            arrival(sb, 0, cc, k, kcols(k), s_send, s_recv).wait_recv()
        q_oth = sb[0, oth_rows, kcols(k)] - pull * pb[0, oth_rows, kcols(k)]
        ob[0, :, kcols(k)] = of_chip(0, k) + product(k_oth, q_oth)
        first_out(k).start()
        out_ref[:, cols(c, h, k, piece)] = ob[0, mine(c), kcols(k)]
        return carry

    lax.fori_loop(0, PARTS, first_step, 0)
    sib_copy(0, 1).wait_recv()
    sib_copy(1, 1).wait_recv()

    def base_step(k, carry):
        ob[1, :, kcols(k)] = of_chip(1, k)
        return carry

    lax.fori_loop(0, PARTS, base_step, 0)

    for k in range(PARTS):
        for cc in range(2):
            p_copy(cc, k).wait_send()
            s_copy(cc, k).wait_send()
    for n in range(2):
        for gi in range(2):
            sib_copy(n, gi).wait_send()
    copy.wait_send()
    on_y(lambda cp: cp.wait_send(), receiver)
    for cp in (*x_copies, *z_copies, *gz_copies, *gx_copies, gc_copy):
        cp.wait_send()
    for k in range(PARTS):
        first_out(k).wait()

    for n in range(len(LAST)):
        for cc in range(2):
            if n:
                q_copy(cc, n - 1).wait_send()
            arrival(sb, 1, cc, n, last_at[n], q_send, q_recv).wait_recv()
        q_oth = sb[1, oth_rows, last_at[n]]
        where, away = last_out(n)
        ob[1, mine(1 - c), last_at[n]] = ob[1, mine(1 - c), last_at[n]] + product(k_oth.at[mine(1 - c), :], q_oth)
        away.start()
        out_ref[:, where] = ob[1, mine(c), last_at[n]] + product(k_oth.at[mine(c), :], q_oth)

    for cc in range(2):
        q_copy(cc, len(LAST) - 1).wait_send()
    for n in range(len(LAST)):
        last_out(n)[1].wait()


def solution(mesh):
    size_dom = mesh.shape["dom"]

    def on_device(particles, scores, spread, step_size):
        rows, width = particles.shape
        quarter = width // 4
        piece = quarter // PARTS
        count = size_dom * rows
        dma = pltpu.SemaphoreType.DMA
        f32 = jnp.float32
        return pl.pallas_call(
            functools.partial(body, size_dom, rows, quarter),
            out_shape=jax.ShapeDtypeStruct(particles.shape, f32),
            in_specs=[pl.BlockSpec(memory_space=pltpu.SMEM), pl.BlockSpec(memory_space=pltpu.SMEM), pl.BlockSpec(memory_space=pltpu.HBM),
                      pl.BlockSpec(memory_space=pltpu.HBM)],
            out_specs=pl.BlockSpec(memory_space=pltpu.VMEM),
            scratch_shapes=[
                pltpu.VMEM((2, count, quarter), f32),
                pltpu.VMEM((2, count, quarter), f32),
                pltpu.VMEM((2, rows, quarter), f32),
                pltpu.VMEM((2, rows, quarter), f32),
                pltpu.VMEM((2, rows, piece), f32),
                pltpu.VMEM((2, 2 * rows, quarter), f32),
                pltpu.VMEM((count, count), f32),
                pltpu.VMEM((count // 2, count), f32),
                pltpu.VMEM((4, count // 8, count), f32),
                pltpu.VMEM((4, count // 32, count), f32),
                pltpu.VMEM((3, count // 32, count), f32),
                pltpu.VMEM((count, count), f32),
                pltpu.VMEM((2 * rows, 2 * rows), f32),
                pltpu.VMEM((2 * rows, 2 * rows), f32),
                pltpu.VMEM((2 * rows, 128), f32),
                dma((10,)), dma((2, 2)), dma((2, 2)),
                dma((2, PARTS)), dma((2, PARTS)), dma((2, PARTS)), dma((2, PARTS)),
                dma((2, len(LAST))), dma((2, len(LAST))),
                dma, dma, dma((3,)), dma((3,)), dma((3,)), dma((3,)), dma((3,)), dma((3,)),
                dma((3,)), dma((3,)), dma((3,)), dma((3,)), dma, dma,
                dma((PARTS + len(LAST),)), dma((PARTS + len(LAST),)),
                pltpu.SemaphoreType.REGULAR,
            ],
            compiler_params=pltpu.CompilerParams(
                collective_id=0, has_side_effects=True, vmem_limit_bytes=48 << 20),
            name="svgd",
        )(spread.reshape(1), step_size.reshape(1), particles, scores)

    return jax.shard_map(
        on_device,
        mesh=mesh,
        in_specs=(P("dom", "dim"), P("dom", "dim"), P(), P()),
        out_specs=P("dom", "dim"),
        check_vma=False,
    )
```

```python
import functools

import jax
import jax.numpy as jnp
from jax import lax
from jax.experimental import pallas as pl
from jax.experimental.pallas import tpu as pltpu
from jax.sharding import PartitionSpec as P

MESH = pl.DeviceIdType.MESH
PARTS = 2
EARLY = 2
LAST = (8, 4, 2, 1, 1)


def body(
    size_dom, rows, quarter,
    spread_ref, step_ref, p_ref, s_ref, out_ref,
    pb, sb, pt, qs, first, ob, gram, half_in, xin, zin, yin, full, k_own, k_oth, w_ref,
    load_sem, sib_send, sib_recv, p_send, p_recv, s_send, s_recv, q_send, q_recv,
    red_send, red_recv, x_send, x_recv, z_send, z_recv, y_send, y_recv,
    gz_send, gz_recv, gx_send, gx_recv, gc_send, gc_recv,
    o_send, o_recv, met,
):
    piece, unit = quarter // PARTS, quarter // 16
    dom, dim = lax.axis_index("dom"), lax.axis_index("dim")
    h, c = dom // 2, lax.rem(dom, 2)
    z, lo, x = dim // 8, lax.rem(dim // 4, 2), lax.rem(dim, 4)
    y = h * 2 + lo
    block = dom

    def dev(hh, cc, zz, ll, xx):
        return (hh * 2 + cc, zz * 8 + ll * 4 + xx)

    sib = dev(h, 1 - c, z, lo, x)
    over = [dev(1 - h, cc, z, lo, x) for cc in range(2)]
    xs = [dev(h, c, z, lo, lax.rem(x + d, 4)) for d in (1, 2, 3)]
    zs = [dev(h, c, lax.rem(z + d, 4), lo, x) for d in (1, 2, 3)]
    ys = []
    for d in (1, 2, 3):
        yy = lax.rem(y + d, 4)
        ys.append(dev(yy // 2, c, z, lax.rem(yy, 2), x))

    ahead = [pltpu.make_async_copy(p_ref.at[:, pl.ds(pl.multiple_of(cc * (2 * quarter) + (1 - h) * quarter, piece), piece)],
                                   first.at[cc], load_sem.at[8 + cc]) for cc in range(2)]
    for load in ahead:
        load.start()

    barrier = pltpu.get_barrier_semaphore()
    near = [sib, *over]
    wide = [*xs, *zs, ys[0], ys[2]]
    for peer in near:
        pl.semaphore_signal(barrier, inc=1, device_id=peer, device_id_type=MESH)

    @pl.when(c == 0)
    def _():
        for peer in wide:
            pl.semaphore_signal(barrier, inc=1, device_id=peer, device_id_type=MESH)
        pl.semaphore_wait(barrier, len(near) + len(wide))

    @pl.when(c == 1)
    def _():
        pl.semaphore_wait(barrier, len(near))

    def remote(src, dst, ssem, rsem, to):
        return pltpu.make_async_remote_copy(
            src_ref=src, dst_ref=dst, send_sem=ssem, recv_sem=rsem,
            device_id=to, device_id_type=MESH,
        )

    def cols(cc, g, k, width):
        return pl.ds(pl.multiple_of(cc * (2 * quarter) + g * quarter + k * piece, piece), width)

    def mine(b):
        return pl.ds(pl.multiple_of(b * rows, rows), rows)

    def kcols(k):
        return pl.ds(pl.multiple_of(k * piece, piece), piece)

    side = [h, 1 - h]

    def p_copy(cc, k):
        source = first.at[cc] if k == 0 else p_ref.at[:, cols(cc, 1 - h, k, piece)]
        return remote(source, pb.at[0, mine(block), kcols(k)],
                      p_send.at[cc, k], p_recv.at[c, k], over[cc])

    def s_copy(cc, k):
        return remote(s_ref.at[:, cols(cc, 1 - h, k, piece)], sb.at[0, mine(block), kcols(k)],
                      s_send.at[cc, k], s_recv.at[c, k], over[cc])

    last_at = [pl.ds(unit * sum(LAST[:n]), unit * width) for n, width in enumerate(LAST)]

    def q_copy(cc, n):
        return remote(qs.at[cc, :, last_at[n]], sb.at[1, mine(block), last_at[n]],
                      q_send.at[cc, n], q_recv.at[c, n], over[cc])

    def arrival(buf, gi, cc, k, at, ssem, rsem):
        there = buf.at[gi, mine((1 - h) * 2 + cc), at]
        return remote(there, there, ssem.at[cc, k], rsem.at[cc, k], over[cc])

    def sib_copy(n, gi):
        src, dst = ((p_ref, pb), (s_ref, sb))[n]
        return remote(src.at[:, cols(1 - c, side[gi], 0, quarter)], dst.at[gi, mine(block), :],
                      sib_send.at[n, gi], sib_recv.at[n, gi], sib)

    for k in range(PARTS):
        for cc in range(2):
            if k == 0:
                ahead[cc].wait()
            p_copy(cc, k).start()
    @pl.when(c == 0)
    def _():
        for peer in wide:
            pl.semaphore_signal(met, inc=1, device_id=peer, device_id_type=MESH)

    loads = []
    for n, (src, dst) in enumerate(((p_ref, pb), (s_ref, sb))):
        for gi in range(2):
            loads.append(pltpu.make_async_copy(
                src.at[:, cols(c, side[gi], 0, quarter)], dst.at[gi, mine(block), :], load_sem.at[2 * n + gi]))
    for cc in range(2):
        loads.append(pltpu.make_async_copy(p_ref.at[:, cols(cc, h, 0, quarter)], pt.at[cc], load_sem.at[4 + cc]))
        loads.append(pltpu.make_async_copy(s_ref.at[:, cols(cc, h, 0, quarter)], qs.at[cc], load_sem.at[6 + cc]))
    for n in range(2):
        for gi in range(2):
            sib_copy(n, gi).start()
    for load in loads:
        load.start()
    for k in range(EARLY):
        for cc in range(2):
            s_copy(cc, k).start()
    for load in loads:
        load.wait()

    spread = jnp.full((1, 128), spread_ref[0], jnp.float32)
    pull = (2.0 / spread)[:, :1]
    for cc in range(2):
        def scale(k, carry, cc=cc):
            qs[cc, :, kcols(k)] = qs[cc, :, kcols(k)] - pull * pt[cc, :, kcols(k)]
            return carry
        lax.fori_loop(0, PARTS, scale, 0)

    sib_copy(0, 0).wait_recv()
    gram[...] = jnp.zeros_like(gram)

    def gram_step(k, carry):
        for cc in range(2):
            arrival(pb, 0, cc, k, kcols(k), p_send, p_recv).wait_recv()
        part = pb[0, :, kcols(k)]
        gram[...] += lax.dot_general(part, part, (((1,), (1,)), ((), ())),
                                     precision=lax.Precision.HIGHEST, preferred_element_type=jnp.float32)
        return carry

    lax.fori_loop(0, PARTS, gram_step, 0)

    count = size_dom * rows
    n_c, n_x, n_z = count // 2, count // 8, count // 32

    def span(start, size):
        return pl.ds(pl.multiple_of(start, size), size)

    @pl.when(c == 0)
    def _():
        pl.semaphore_wait(met, len(wide))
        pl.semaphore_signal(met, inc=1, device_id=sib, device_id_type=MESH)

    @pl.when(c == 1)
    def _():
        pl.semaphore_wait(met, 1)

    copy = remote(gram.at[span((1 - c) * n_c, n_c), :], half_in, red_send, red_recv, sib)
    copy.start()
    copy.wait_recv()
    half_in[...] += gram[span(c * n_c, n_c), :]
    x_copies = [remote(half_in.at[span(lax.rem(x + d, 4) * n_x, n_x), :], xin.at[d - 1],
                       x_send.at[d - 1], x_recv.at[d - 1], xs[d - 1]) for d in (1, 2, 3)]
    for cp in x_copies:
        cp.start()
    for cp in x_copies:
        cp.wait_recv()
    xin[3] = half_in[span(x * n_x, n_x), :] + xin[0] + xin[1] + xin[2]
    z_copies = [remote(xin.at[3, span(lax.rem(z + d, 4) * n_z, n_z), :], zin.at[d - 1],
                       z_send.at[d - 1], z_recv.at[d - 1], zs[d - 1]) for d in (1, 2, 3)]
    for cp in z_copies:
        cp.start()
    for cp in z_copies:
        cp.wait_recv()
    zin[3] = xin[3, span(z * n_z, n_z), :] + zin[0] + zin[1] + zin[2]
    tile = pl.ds(pl.multiple_of((c * 2 + x // 2) * 128, 128), 128)

    def y_copy(d, whole):
        src, dst = zin.at[3], yin.at[d - 1]
        if not whole:
            src, dst = src.at[:, tile], dst.at[:, tile]
        return remote(src, dst, y_send.at[d - 1], y_recv.at[d - 1], ys[d - 1])

    def on_y(act, of):
        for d in (1, 2, 3):
            use = of(d)

            @pl.when(use == c)
            def _(d=d):
                act(y_copy(d, True))

            @pl.when(use != c)
            def _(d=d):
                act(y_copy(d, False))

    def receiver(d):
        return lax.rem(y + d, 4) // 2

    on_y(lambda cp: cp.start(), receiver)
    for k in range(EARLY, PARTS):
        for cc in range(2):
            s_copy(cc, k).start()
    for n in range(len(LAST)):
        for cc in range(2):
            q_copy(cc, n).start()
    on_y(lambda cp: cp.wait_recv(), lambda d: h)
    at_z = span(c * n_c + x * n_x + z * n_z, n_z)
    at_x = span(c * n_c + x * n_x, n_x)
    at_c = span(c * n_c, n_c)

    @pl.when(h == c)
    def _():
        full[at_z, :] = zin[3] + yin[0] + yin[1] + yin[2]

    @pl.when(h != c)
    def _():
        full[at_z, :] = zin[3]
        full[at_z, tile] = zin[3, :, tile] + yin[0, :, tile] + yin[1, :, tile] + yin[2, :, tile]

    gz_copies = [remote(full.at[at_z, :], full.at[at_z, :], gz_send.at[d - 1], gz_recv.at[d - 1], zs[d - 1])
                 for d in (1, 2, 3)]
    for cp in gz_copies:
        cp.start()
    for cp in gz_copies:
        cp.wait_recv()
    gx_copies = [remote(full.at[at_x, :], full.at[at_x, :], gx_send.at[d - 1], gx_recv.at[d - 1], xs[d - 1])
                 for d in (1, 2, 3)]
    for cp in gx_copies:
        cp.start()
    for cp in gx_copies:
        cp.wait_recv()
    gc_copy = remote(full.at[at_c, :], full.at[at_c, :], gc_send, gc_recv, sib)
    gc_copy.start()
    gc_copy.wait_recv()

    pair = 2 * rows
    one = spread[:, :1]

    def diagonal(size, row0, col0, axis):
        tile = full[span(row0, size), :] if axis == 1 else full[...]
        r = lax.broadcasted_iota(jnp.int32, tile.shape, 0) + row0
        q = lax.broadcasted_iota(jnp.int32, tile.shape, 1)
        return jnp.sum(jnp.where(r == q, tile, 0.0), axis=axis, keepdims=True)

    own_sq = diagonal(pair, h * pair, 0, 1)
    all_sq = diagonal(count, 0, 0, 0)
    kern = jnp.exp(-(own_sq + all_sq - 2.0 * full[span(h * pair, pair), :]) / one)
    step = jnp.full((1, 128), step_ref[0], jnp.float32)[:, :1]
    gain = step / jnp.float32(count)
    w_ref[...] = jnp.broadcast_to(1.0 + gain * pull * jnp.sum(kern, axis=1, keepdims=True), w_ref.shape)
    kern = gain * kern
    low, high = kern[:, :pair], kern[:, pair:]
    upper = h == 0
    k_own[...] = jnp.where(upper, low, high)
    k_oth[...] = jnp.where(upper, high, low)
    own_rows, oth_rows = span(h * pair, pair), span((1 - h) * pair, pair)

    def product(k_ref, value):
        return jnp.dot(k_ref[...], value, precision=lax.Precision.HIGHEST, preferred_element_type=jnp.float32)

    def of_chip(gi, k):
        particles = pb[gi, own_rows, kcols(k)]
        return w_ref[:, :1] * particles + product(k_own, sb[gi, own_rows, kcols(k)] - pull * particles)

    def first_out(k):
        return remote(ob.at[0, mine(1 - c), kcols(k)], out_ref.at[:, cols(c, h, k, piece)],
                      o_send.at[k], o_recv.at[k], sib)

    def last_out(n):
        where = pl.ds(pl.multiple_of(c * (2 * quarter) + (1 - h) * quarter + unit * sum(LAST[:n]), unit), unit * LAST[n])
        return where, remote(ob.at[1, mine(1 - c), last_at[n]], out_ref.at[:, where],
                             o_send.at[PARTS + n], o_recv.at[PARTS + n], sib)

    sib_copy(1, 0).wait_recv()

    def first_step(k, carry):
        for cc in range(2):
            arrival(sb, 0, cc, k, kcols(k), s_send, s_recv).wait_recv()
        q_oth = sb[0, oth_rows, kcols(k)] - pull * pb[0, oth_rows, kcols(k)]
        ob[0, :, kcols(k)] = of_chip(0, k) + product(k_oth, q_oth)
        first_out(k).start()
        out_ref[:, cols(c, h, k, piece)] = ob[0, mine(c), kcols(k)]
        return carry

    lax.fori_loop(0, PARTS, first_step, 0)
    sib_copy(0, 1).wait_recv()
    sib_copy(1, 1).wait_recv()

    def base_step(k, carry):
        ob[1, :, kcols(k)] = of_chip(1, k)
        return carry

    lax.fori_loop(0, PARTS, base_step, 0)
    for n in range(len(LAST)):
        for cc in range(2):
            arrival(sb, 1, cc, n, last_at[n], q_send, q_recv).wait_recv()
        q_oth = sb[1, oth_rows, last_at[n]]
        where, away = last_out(n)
        ob[1, mine(1 - c), last_at[n]] = ob[1, mine(1 - c), last_at[n]] + product(k_oth.at[mine(1 - c), :], q_oth)
        away.start()
        out_ref[:, where] = ob[1, mine(c), last_at[n]] + product(k_oth.at[mine(c), :], q_oth)

    for k in range(PARTS):
        for cc in range(2):
            p_copy(cc, k).wait_send()
            s_copy(cc, k).wait_send()
    for n in range(len(LAST)):
        for cc in range(2):
            q_copy(cc, n).wait_send()
    for n in range(2):
        for gi in range(2):
            sib_copy(n, gi).wait_send()
    copy.wait_send()
    on_y(lambda cp: cp.wait_send(), receiver)
    for cp in (*x_copies, *z_copies, *gz_copies, *gx_copies, gc_copy):
        cp.wait_send()
    for k in range(PARTS):
        first_out(k).wait()
    for n in range(len(LAST)):
        last_out(n)[1].wait()


def solution(mesh):
    size_dom = mesh.shape["dom"]

    def on_device(particles, scores, spread, step_size):
        rows, width = particles.shape
        quarter = width // 4
        piece = quarter // PARTS
        count = size_dom * rows
        dma = pltpu.SemaphoreType.DMA
        f32 = jnp.float32
        return pl.pallas_call(
            functools.partial(body, size_dom, rows, quarter),
            out_shape=jax.ShapeDtypeStruct(particles.shape, f32),
            in_specs=[pl.BlockSpec(memory_space=pltpu.SMEM), pl.BlockSpec(memory_space=pltpu.SMEM), pl.BlockSpec(memory_space=pltpu.HBM),
                      pl.BlockSpec(memory_space=pltpu.HBM)],
            out_specs=pl.BlockSpec(memory_space=pltpu.VMEM),
            scratch_shapes=[
                pltpu.VMEM((2, count, quarter), f32),
                pltpu.VMEM((2, count, quarter), f32),
                pltpu.VMEM((2, rows, quarter), f32),
                pltpu.VMEM((2, rows, quarter), f32),
                pltpu.VMEM((2, rows, piece), f32),
                pltpu.VMEM((2, 2 * rows, quarter), f32),
                pltpu.VMEM((count, count), f32),
                pltpu.VMEM((count // 2, count), f32),
                pltpu.VMEM((4, count // 8, count), f32),
                pltpu.VMEM((4, count // 32, count), f32),
                pltpu.VMEM((3, count // 32, count), f32),
                pltpu.VMEM((count, count), f32),
                pltpu.VMEM((2 * rows, 2 * rows), f32),
                pltpu.VMEM((2 * rows, 2 * rows), f32),
                pltpu.VMEM((2 * rows, 128), f32),
                dma((10,)), dma((2, 2)), dma((2, 2)),
                dma((2, PARTS)), dma((2, PARTS)), dma((2, PARTS)), dma((2, PARTS)),
                dma((2, len(LAST))), dma((2, len(LAST))),
                dma, dma, dma((3,)), dma((3,)), dma((3,)), dma((3,)), dma((3,)), dma((3,)),
                dma((3,)), dma((3,)), dma((3,)), dma((3,)), dma, dma,
                dma((PARTS + len(LAST),)), dma((PARTS + len(LAST),)),
                pltpu.SemaphoreType.REGULAR,
            ],
            compiler_params=pltpu.CompilerParams(
                collective_id=0, has_side_effects=True, vmem_limit_bytes=48 << 20),
            name="svgd",
        )(spread.reshape(1), step_size.reshape(1), particles, scores)

    return jax.shard_map(
        on_device,
        mesh=mesh,
        in_specs=(P("dom", "dim"), P("dom", "dim"), P(), P()),
        out_specs=P("dom", "dim"),
        check_vma=False,
    )
```

```python
import functools

import jax
import jax.numpy as jnp
from jax import lax
from jax.experimental import pallas as pl
from jax.experimental.pallas import tpu as pltpu
from jax.sharding import PartitionSpec as P

MESH = pl.DeviceIdType.MESH
PARTS = 2
EARLY = 2
LAST = (8, 4, 2, 1, 1)


def body(
    size_dom, rows, quarter,
    spread_ref, step_ref, p_ref, s_ref, out_ref,
    pb, sb, pt, qs, first, ob, gram, half_in, xin, zin, yin, full, k_own, k_oth, w_ref,
    load_sem, sib_send, sib_recv, p_send, p_recv, s_send, s_recv, q_send, q_recv,
    red_send, red_recv, x_send, x_recv, z_send, z_recv, y_send, y_recv,
    gz_send, gz_recv, gx_send, gx_recv, gc_send, gc_recv,
    o_send, o_recv, met,
):
    piece, unit = quarter // PARTS, quarter // 16
    dom, dim = lax.axis_index("dom"), lax.axis_index("dim")
    h, c = dom // 2, lax.rem(dom, 2)
    z, lo, x = dim // 8, lax.rem(dim // 4, 2), lax.rem(dim, 4)
    y = h * 2 + lo
    block = dom

    def dev(hh, cc, zz, ll, xx):
        return (hh * 2 + cc, zz * 8 + ll * 4 + xx)

    sib = dev(h, 1 - c, z, lo, x)
    over = [dev(1 - h, cc, z, lo, x) for cc in range(2)]
    xs = [dev(h, c, z, lo, lax.rem(x + d, 4)) for d in (1, 2, 3)]
    zs = [dev(h, c, lax.rem(z + d, 4), lo, x) for d in (1, 2, 3)]
    ys = []
    for d in (1, 2, 3):
        yy = lax.rem(y + d, 4)
        ys.append(dev(yy // 2, c, z, lax.rem(yy, 2), x))

    ahead = [pltpu.make_async_copy(p_ref.at[:, pl.ds(pl.multiple_of(cc * (2 * quarter) + (1 - h) * quarter, piece), piece)],
                                   first.at[cc], load_sem.at[8 + cc]) for cc in range(2)]
    for load in ahead:
        load.start()

    barrier = pltpu.get_barrier_semaphore()
    near = [sib, *over]
    wide = [*xs, *zs, ys[0], ys[2]]
    for peer in near:
        pl.semaphore_signal(barrier, inc=1, device_id=peer, device_id_type=MESH)

    @pl.when(c == 0)
    def _():
        for peer in wide:
            pl.semaphore_signal(barrier, inc=1, device_id=peer, device_id_type=MESH)
        pl.semaphore_wait(barrier, len(near) + len(wide))

    @pl.when(c == 1)
    def _():
        pl.semaphore_wait(barrier, len(near))

    def remote(src, dst, ssem, rsem, to):
        return pltpu.make_async_remote_copy(
            src_ref=src, dst_ref=dst, send_sem=ssem, recv_sem=rsem,
            device_id=to, device_id_type=MESH,
        )

    def cols(cc, g, k, width):
        return pl.ds(pl.multiple_of(cc * (2 * quarter) + g * quarter + k * piece, piece), width)

    def mine(b):
        return pl.ds(pl.multiple_of(b * rows, rows), rows)

    def kcols(k):
        return pl.ds(pl.multiple_of(k * piece, piece), piece)

    side = [h, 1 - h]

    def p_copy(cc, k):
        source = first.at[cc] if k == 0 else p_ref.at[:, cols(cc, 1 - h, k, piece)]
        return remote(source, pb.at[0, mine(block), kcols(k)],
                      p_send.at[cc, k], p_recv.at[c, k], over[cc])

    def s_copy(cc, k):
        return remote(s_ref.at[:, cols(cc, 1 - h, k, piece)], sb.at[0, mine(block), kcols(k)],
                      s_send.at[cc, k], s_recv.at[c, k], over[cc])

    last_at = [pl.ds(unit * sum(LAST[:n]), unit * width) for n, width in enumerate(LAST)]

    def q_copy(cc, n):
        return remote(qs.at[cc, :, last_at[n]], sb.at[1, mine(block), last_at[n]],
                      q_send.at[cc, n], q_recv.at[c, n], over[cc])

    def arrival(buf, gi, cc, k, at, ssem, rsem):
        there = buf.at[gi, mine((1 - h) * 2 + cc), at]
        return remote(there, there, ssem.at[cc, k], rsem.at[cc, k], over[cc])

    def sib_copy(n, gi):
        src, dst = ((p_ref, pb), (s_ref, sb))[n]
        return remote(src.at[:, cols(1 - c, side[gi], 0, quarter)], dst.at[gi, mine(block), :],
                      sib_send.at[n, gi], sib_recv.at[n, gi], sib)

    for k in range(PARTS):
        for cc in range(2):
            if k == 0:
                ahead[cc].wait()
            p_copy(cc, k).start()
    @pl.when(c == 0)
    def _():
        for peer in wide:
            pl.semaphore_signal(met, inc=1, device_id=peer, device_id_type=MESH)

    loads = []
    for n, (src, dst) in enumerate(((p_ref, pb), (s_ref, sb))):
        for gi in range(2):
            loads.append(pltpu.make_async_copy(
                src.at[:, cols(c, side[gi], 0, quarter)], dst.at[gi, mine(block), :], load_sem.at[2 * n + gi]))
    for cc in range(2):
        loads.append(pltpu.make_async_copy(p_ref.at[:, cols(cc, h, 0, quarter)], pt.at[cc], load_sem.at[4 + cc]))
        loads.append(pltpu.make_async_copy(s_ref.at[:, cols(cc, h, 0, quarter)], qs.at[cc], load_sem.at[6 + cc]))
    for n in range(2):
        for gi in range(2):
            sib_copy(n, gi).start()
    for load in loads:
        load.start()
    for k in range(EARLY):
        for cc in range(2):
            s_copy(cc, k).start()
    for load in loads:
        load.wait()

    spread = jnp.full((1, 128), spread_ref[()], jnp.float32)
    pull = (2.0 / spread)[:, :1]
    for cc in range(2):
        def scale(k, carry, cc=cc):
            qs[cc, :, kcols(k)] = qs[cc, :, kcols(k)] - pull * pt[cc, :, kcols(k)]
            return carry
        lax.fori_loop(0, PARTS, scale, 0)

    sib_copy(0, 0).wait_recv()
    gram[...] = jnp.zeros_like(gram)

    def gram_step(k, carry):
        for cc in range(2):
            arrival(pb, 0, cc, k, kcols(k), p_send, p_recv).wait_recv()
        part = pb[0, :, kcols(k)]
        gram[...] += lax.dot_general(part, part, (((1,), (1,)), ((), ())),
                                     precision=lax.Precision.HIGHEST, preferred_element_type=jnp.float32)
        return carry

    lax.fori_loop(0, PARTS, gram_step, 0)

    count = size_dom * rows
    n_c, n_x, n_z = count // 2, count // 8, count // 32

    def span(start, size):
        return pl.ds(pl.multiple_of(start, size), size)

    @pl.when(c == 0)
    def _():
        pl.semaphore_wait(met, len(wide))
        pl.semaphore_signal(met, inc=1, device_id=sib, device_id_type=MESH)

    @pl.when(c == 1)
    def _():
        pl.semaphore_wait(met, 1)

    copy = remote(gram.at[span((1 - c) * n_c, n_c), :], half_in, red_send, red_recv, sib)
    copy.start()
    copy.wait_recv()
    half_in[...] += gram[span(c * n_c, n_c), :]
    x_copies = [remote(half_in.at[span(lax.rem(x + d, 4) * n_x, n_x), :], xin.at[d - 1],
                       x_send.at[d - 1], x_recv.at[d - 1], xs[d - 1]) for d in (1, 2, 3)]
    for cp in x_copies:
        cp.start()
    for cp in x_copies:
        cp.wait_recv()
    xin[3] = half_in[span(x * n_x, n_x), :] + xin[0] + xin[1] + xin[2]
    z_copies = [remote(xin.at[3, span(lax.rem(z + d, 4) * n_z, n_z), :], zin.at[d - 1],
                       z_send.at[d - 1], z_recv.at[d - 1], zs[d - 1]) for d in (1, 2, 3)]
    for cp in z_copies:
        cp.start()
    for cp in z_copies:
        cp.wait_recv()
    zin[3] = xin[3, span(z * n_z, n_z), :] + zin[0] + zin[1] + zin[2]
    tile = pl.ds(pl.multiple_of((c * 2 + x // 2) * 128, 128), 128)

    def y_copy(d, whole):
        src, dst = zin.at[3], yin.at[d - 1]
        if not whole:
            src, dst = src.at[:, tile], dst.at[:, tile]
        return remote(src, dst, y_send.at[d - 1], y_recv.at[d - 1], ys[d - 1])

    def on_y(act, of):
        for d in (1, 2, 3):
            use = of(d)

            @pl.when(use == c)
            def _(d=d):
                act(y_copy(d, True))

            @pl.when(use != c)
            def _(d=d):
                act(y_copy(d, False))

    def receiver(d):
        return lax.rem(y + d, 4) // 2

    on_y(lambda cp: cp.start(), receiver)
    for k in range(EARLY, PARTS):
        for cc in range(2):
            s_copy(cc, k).start()
    for n in range(len(LAST)):
        for cc in range(2):
            q_copy(cc, n).start()
    on_y(lambda cp: cp.wait_recv(), lambda d: h)
    at_z = span(c * n_c + x * n_x + z * n_z, n_z)
    at_x = span(c * n_c + x * n_x, n_x)
    at_c = span(c * n_c, n_c)

    @pl.when(h == c)
    def _():
        full[at_z, :] = zin[3] + yin[0] + yin[1] + yin[2]

    @pl.when(h != c)
    def _():
        full[at_z, :] = zin[3]
        full[at_z, tile] = zin[3, :, tile] + yin[0, :, tile] + yin[1, :, tile] + yin[2, :, tile]

    gz_copies = [remote(full.at[at_z, :], full.at[at_z, :], gz_send.at[d - 1], gz_recv.at[d - 1], zs[d - 1])
                 for d in (1, 2, 3)]
    for cp in gz_copies:
        cp.start()
    for cp in gz_copies:
        cp.wait_recv()
    gx_copies = [remote(full.at[at_x, :], full.at[at_x, :], gx_send.at[d - 1], gx_recv.at[d - 1], xs[d - 1])
                 for d in (1, 2, 3)]
    for cp in gx_copies:
        cp.start()
    for cp in gx_copies:
        cp.wait_recv()
    gc_copy = remote(full.at[at_c, :], full.at[at_c, :], gc_send, gc_recv, sib)
    gc_copy.start()
    gc_copy.wait_recv()

    pair = 2 * rows
    one = spread[:, :1]

    def diagonal(size, row0, col0, axis):
        tile = full[span(row0, size), :] if axis == 1 else full[...]
        r = lax.broadcasted_iota(jnp.int32, tile.shape, 0) + row0
        q = lax.broadcasted_iota(jnp.int32, tile.shape, 1)
        return jnp.sum(jnp.where(r == q, tile, 0.0), axis=axis, keepdims=True)

    own_sq = diagonal(pair, h * pair, 0, 1)
    all_sq = diagonal(count, 0, 0, 0)
    kern = jnp.exp(-(own_sq + all_sq - 2.0 * full[span(h * pair, pair), :]) / one)
    step = jnp.full((1, 128), step_ref[()], jnp.float32)[:, :1]
    gain = step / jnp.float32(count)
    w_ref[...] = jnp.broadcast_to(1.0 + gain * pull * jnp.sum(kern, axis=1, keepdims=True), w_ref.shape)
    kern = gain * kern
    low, high = kern[:, :pair], kern[:, pair:]
    upper = h == 0
    k_own[...] = jnp.where(upper, low, high)
    k_oth[...] = jnp.where(upper, high, low)
    own_rows, oth_rows = span(h * pair, pair), span((1 - h) * pair, pair)

    def product(k_ref, value):
        return jnp.dot(k_ref[...], value, precision=lax.Precision.HIGHEST, preferred_element_type=jnp.float32)

    def of_chip(gi, k):
        particles = pb[gi, own_rows, kcols(k)]
        return w_ref[:, :1] * particles + product(k_own, sb[gi, own_rows, kcols(k)] - pull * particles)

    def first_out(k):
        return remote(ob.at[0, mine(1 - c), kcols(k)], out_ref.at[:, cols(c, h, k, piece)],
                      o_send.at[k], o_recv.at[k], sib)

    def last_out(n):
        where = pl.ds(pl.multiple_of(c * (2 * quarter) + (1 - h) * quarter + unit * sum(LAST[:n]), unit), unit * LAST[n])
        return where, remote(ob.at[1, mine(1 - c), last_at[n]], out_ref.at[:, where],
                             o_send.at[PARTS + n], o_recv.at[PARTS + n], sib)

    sib_copy(1, 0).wait_recv()

    def first_step(k, carry):
        for cc in range(2):
            arrival(sb, 0, cc, k, kcols(k), s_send, s_recv).wait_recv()
        q_oth = sb[0, oth_rows, kcols(k)] - pull * pb[0, oth_rows, kcols(k)]
        ob[0, :, kcols(k)] = of_chip(0, k) + product(k_oth, q_oth)
        first_out(k).start()
        out_ref[:, cols(c, h, k, piece)] = ob[0, mine(c), kcols(k)]
        return carry

    lax.fori_loop(0, PARTS, first_step, 0)
    sib_copy(0, 1).wait_recv()
    sib_copy(1, 1).wait_recv()

    def base_step(k, carry):
        ob[1, :, kcols(k)] = of_chip(1, k)
        return carry

    lax.fori_loop(0, PARTS, base_step, 0)
    for n in range(len(LAST)):
        for cc in range(2):
            arrival(sb, 1, cc, n, last_at[n], q_send, q_recv).wait_recv()
        q_oth = sb[1, oth_rows, last_at[n]]
        where, away = last_out(n)
        ob[1, mine(1 - c), last_at[n]] = ob[1, mine(1 - c), last_at[n]] + product(k_oth.at[mine(1 - c), :], q_oth)
        away.start()
        out_ref[:, where] = ob[1, mine(c), last_at[n]] + product(k_oth.at[mine(c), :], q_oth)

    for k in range(PARTS):
        for cc in range(2):
            p_copy(cc, k).wait_send()
            s_copy(cc, k).wait_send()
    for n in range(len(LAST)):
        for cc in range(2):
            q_copy(cc, n).wait_send()
    for n in range(2):
        for gi in range(2):
            sib_copy(n, gi).wait_send()
    copy.wait_send()
    on_y(lambda cp: cp.wait_send(), receiver)
    for cp in (*x_copies, *z_copies, *gz_copies, *gx_copies, gc_copy):
        cp.wait_send()
    for k in range(PARTS):
        first_out(k).wait()
    for n in range(len(LAST)):
        last_out(n)[1].wait()


def solution(mesh):
    size_dom = mesh.shape["dom"]

    def on_device(particles, scores, spread, step_size):
        rows, width = particles.shape
        quarter = width // 4
        piece = quarter // PARTS
        count = size_dom * rows
        dma = pltpu.SemaphoreType.DMA
        f32 = jnp.float32
        return pl.pallas_call(
            functools.partial(body, size_dom, rows, quarter),
            out_shape=jax.ShapeDtypeStruct(particles.shape, f32),
            in_specs=[pl.BlockSpec(memory_space=pltpu.SMEM), pl.BlockSpec(memory_space=pltpu.SMEM), pl.BlockSpec(memory_space=pltpu.HBM),
                      pl.BlockSpec(memory_space=pltpu.HBM)],
            out_specs=pl.BlockSpec(memory_space=pltpu.VMEM),
            scratch_shapes=[
                pltpu.VMEM((2, count, quarter), f32),
                pltpu.VMEM((2, count, quarter), f32),
                pltpu.VMEM((2, rows, quarter), f32),
                pltpu.VMEM((2, rows, quarter), f32),
                pltpu.VMEM((2, rows, piece), f32),
                pltpu.VMEM((2, 2 * rows, quarter), f32),
                pltpu.VMEM((count, count), f32),
                pltpu.VMEM((count // 2, count), f32),
                pltpu.VMEM((4, count // 8, count), f32),
                pltpu.VMEM((4, count // 32, count), f32),
                pltpu.VMEM((3, count // 32, count), f32),
                pltpu.VMEM((count, count), f32),
                pltpu.VMEM((2 * rows, 2 * rows), f32),
                pltpu.VMEM((2 * rows, 2 * rows), f32),
                pltpu.VMEM((2 * rows, 128), f32),
                dma((10,)), dma((2, 2)), dma((2, 2)),
                dma((2, PARTS)), dma((2, PARTS)), dma((2, PARTS)), dma((2, PARTS)),
                dma((2, len(LAST))), dma((2, len(LAST))),
                dma, dma, dma((3,)), dma((3,)), dma((3,)), dma((3,)), dma((3,)), dma((3,)),
                dma((3,)), dma((3,)), dma((3,)), dma((3,)), dma, dma,
                dma((PARTS + len(LAST),)), dma((PARTS + len(LAST),)),
                pltpu.SemaphoreType.REGULAR,
            ],
            compiler_params=pltpu.CompilerParams(
                collective_id=0, has_side_effects=True, vmem_limit_bytes=48 << 20),
            name="svgd",
        )(spread, step_size, particles, scores)

    return jax.shard_map(
        on_device,
        mesh=mesh,
        in_specs=(P("dom", "dim"), P("dom", "dim"), P(), P()),
        out_specs=P("dom", "dim"),
        check_vma=False,
    )
```
